32 devices in a mesh: rows: 16 (over z, x, core), cols: 2 (over y).
Axes of the slice: x: 2, y: 2, z: 4, core: 2. Of those that a mesh axis runs over, the one named last changes fastest.
Arguments:
- columns: float32 [512, 16384], P('cols', 'rows'), may hold values from -200 to 200
Outputs:
- orthonormal: float32 [256, 16384], P('cols', 'rows')
- triangle: float32 [256, 512], P('cols')
- trailing: float32 [256, 16384], P('cols', 'rows')
The draws below stay inside these ranges and needn't reach their ends.
All inputs are finite; a program needn't handle non-finite values.
Results may differ from the reference program's by a relative error of at most 0.00008.
Values sent between devices are 32-bit elements; how exact they have to be, the bound alone decides.
A program may use at most 64 MiB of HBM per device.

```python
import math
import jax
import jax.numpy as jnp
from jax import lax

PANEL = 128
COLUMNS = 512
M_ROWS = 16384


def draw_columns(key, part):
    key_normal = jax.random.fold_in(key, 0)
    entries = jnp.clip(jax.random.normal(key_normal, (COLUMNS, M_ROWS), jnp.float32), -4.0, 4.0)
    position = jnp.arange(M_ROWS, dtype=jnp.float32) / max(M_ROWS - 1, 1)
    rising = 1.0 + 2.0 * position
    return (entries * rising[None, :]).astype(jnp.float32)


def setup_inputs(seed: int = 0) -> dict:
    streams_of = jax.random.split(jax.random.key(seed), 2)
    return {
        "columns": draw_columns(jax.random.fold_in(streams_of[1], 71), 0),
    }


precise = lax.Precision.HIGHEST

def product(left, right):
    return jnp.dot(left.astype(jnp.float32), right.astype(jnp.float32), precision=precise, preferred_element_type=jnp.float32)

def gram_matrix(col_block):
    return product(col_block, col_block.T)

def inverse_lower(lower):
    identity = jnp.eye(lower.shape[0], dtype=lower.dtype)
    return lax.linalg.triangular_solve(lower, identity, left_side=True, lower=True)

def reference(columns):
    scaling = math.sqrt(columns.shape[1])
    panel_first = columns[:PANEL]
    remainder = columns[PANEL:]
    lower_first = jnp.linalg.cholesky(gram_matrix(panel_first))
    ortho_first = product(inverse_lower(lower_first), panel_first)
    coupling_first = product(ortho_first, remainder.T)
    remainder = remainder - product(coupling_first.T, ortho_first)
    panel_second = remainder[:PANEL]
    trailing = remainder[PANEL:]
    lower_second = jnp.linalg.cholesky(gram_matrix(panel_second))
    ortho_second = product(inverse_lower(lower_second), panel_second)
    coupling_second = product(ortho_second, trailing.T)
    trailing = trailing - product(coupling_second.T, ortho_second)
    orthonormal = jnp.concatenate([ortho_first, ortho_second], axis=0) * scaling
    zero_block = jnp.zeros((PANEL, PANEL), columns.dtype)
    upper_rows = jnp.concatenate([lower_first.T, coupling_first], axis=1)
    lower_rows = jnp.concatenate([zero_block, lower_second.T, coupling_second], axis=1)
    triangle = jnp.concatenate([upper_rows, lower_rows], axis=0) / scaling
    return (orthonormal, triangle, trailing)
```

```python
import functools
import math

import jax
import jax.numpy as jnp
from jax import lax
from jax.experimental import pallas as pl
from jax.experimental.pallas import tpu as pltpu
from jax.sharding import PartitionSpec as P

PANEL = 128
STRIP = 16
VMEM_BYTES = 20 * 2**20
MESH = pl.DeviceIdType.MESH

precise = lax.Precision.HIGHEST


def product(left, right):
    return jnp.dot(left, right, precision=precise, preferred_element_type=jnp.float32)


def contract(left, right, dims):
    return lax.dot_general(
        left, right, (dims, ((), ())), precision=precise, preferred_element_type=jnp.float32
    )


def across_rows(left, right):
    return contract(left, right, ((1,), (1,)))


def pieces(value):
    first = value.astype(jnp.bfloat16)
    rest = value - first.astype(jnp.float32)
    second = rest.astype(jnp.bfloat16)
    third = (rest - second.astype(jnp.float32)).astype(jnp.bfloat16)
    return first, second, third


def strip_update(left, right):
    a, b, c = pieces(left)
    d, e, f = pieces(right)
    lhs = jnp.concatenate([a, a, b, a, c, b], axis=0)
    rhs = jnp.concatenate([d, e, d, f, d, e], axis=0)
    return lax.dot_general(
        lhs, rhs, (((0,), (0,)), ((), ())), preferred_element_type=jnp.float32
    )


def eliminate(ref, hooks):
    size = ref.shape[0]
    lanes = size
    parts = ref.shape[1] // lanes
    below = lax.broadcasted_iota(jnp.int32, (STRIP, lanes), 0)
    for s in range(size // STRIP):
        at = s * STRIP
        rows = [ref[at:at + STRIP, q * lanes:(q + 1) * lanes] for q in range(parts)]
        cols = [
            jnp.broadcast_to(rows[0][:, at + j:at + j + 1], (STRIP, lanes))
            for j in range(STRIP)
        ]
        for i in range(STRIP):
            pivot = cols[i][i:i + 1]
            inv = lax.rsqrt(pivot)
            inv = inv * (1.5 - 0.5 * pivot * inv * inv)
            col = cols[i] * inv
            coef = jnp.where(below > i, col, 0.0)
            for j in range(i + 1, STRIP):
                cols[j] = cols[j] - coef * col[j:j + 1]
            for q in range(parts):
                row = rows[q][i:i + 1] * inv
                rows[q] = jnp.where(below == i, row, rows[q] - coef * row)
        for q in range(parts):
            ref[at:at + STRIP, q * lanes:(q + 1) * lanes] = rows[q]
        after = at + STRIP
        if after < size:
            update = strip_update(rows[0], jnp.concatenate(rows, axis=1))
            ref[after:, :] = ref[after:, :] - update[after:, :]
        if s in hooks:
            hooks[s]()


def kernel(row_count, scaling, x_ref, q_ref, tail_ref, tri_ref, inv_ref, sum_ref,
           xs, ys, part, gram, pair_in, ring_in, first, second, inverse, power, z_ref,
           xy, xy_pair, xy_ring, xy_all, load, x_send, x_recv, g_send, g_recv,
           y_send, y_recv, relay):
    r = lax.axis_index("rows")
    c = lax.axis_index("cols")
    other = 1 - c
    parity = lax.rem(r, 2)
    h = r // 2
    mates = row_count // 2
    line = mates // 2
    place = h // 2
    partner = (r + 1 - 2 * parity, c)
    across = (r, other)
    side = ((h + 1 - 2 * lax.rem(h, 2)) * 2 + parity, c)
    above = (r + 4, c)
    below = (r - 4, c)
    has_above = place < line - 1
    has_below = place > 0
    size = PANEL
    width = xs.shape[1]
    half_width = width // 2
    eighth = width // 8

    def mate(k):
        return lax.rem(h + k, mates)

    def sender(k):
        return lax.rem(h + mates - k, mates)

    def at(idx, plane):
        return (idx * 2 + parity, plane)

    def push(src, dst, send_sem, recv_sem, target):
        return pltpu.make_async_remote_copy(
            src_ref=src, dst_ref=dst, send_sem=send_sem, recv_sem=recv_sem,
            device_id=target, device_id_type=MESH)

    def signal(sem, target):
        pl.semaphore_signal(sem, inc=1, device_id=target, device_id_type=MESH)

    barrier = pltpu.get_barrier_semaphore()
    for target in (across, partner, side):
        signal(barrier, target)

    @pl.when(has_above)
    def _():
        signal(barrier, above)

    @pl.when(has_below)
    def _():
        signal(barrier, below)

    early = pl.ds(0, half_width)
    late = pl.ds(half_width, half_width)

    def load_copy(q, dst):
        span = early if q == 0 else late
        return pltpu.make_async_copy(x_ref.at[:, span], dst.at[:, span], load.at[q])

    @pl.when(c == 0)
    def _():
        for q in range(2):
            load_copy(q, xs).start()

    @pl.when(c == 1)
    def _():
        for q in range(2):
            load_copy(q, ys).start()

    pl.semaphore_wait(barrier, 3 + has_above.astype(jnp.int32) + has_below.astype(jnp.int32))

    part_rows = size // 2
    top = [pl.ds(q * size, part_rows) for q in range(2)]
    bottom = [pl.ds(q * size + part_rows, part_rows) for q in range(2)]
    every = pl.ds(0, 2 * size)

    def cols(lo, count):
        return pl.ds(lo * eighth, count * eighth)

    x_views = (
        [(rows, late) for rows in top]
        + [(rows, cols(4, 2)) for rows in bottom]
        + [(rows, cols(6, 2)) for rows in bottom]
        + [(every, cols(0, 1)), (pl.ds(0, size), cols(1, 1)), (pl.ds(size, size), cols(1, 1)),
           (every, cols(2, 1)), (every, cols(3, 1))]
    )
    y_views = [(pl.ds(0, size), early), (pl.ds(size, size), early), (pl.ds(0, size), late)]

    def x_copy(q):
        return push(x_ref.at[x_views[q]], xs.at[x_views[q]], x_send.at[q], x_recv.at[q], across)

    def y_copy(q):
        return push(x_ref.at[y_views[q]], ys.at[y_views[q]], x_send.at[q], x_recv.at[q], across)

    @pl.when(c == 0)
    def _():
        for q in range(4):
            x_copy(q).start()

    @pl.when(c == 1)
    def _():
        for q in range(3):
            y_copy(q).start()

    @pl.when(jnp.logical_not(has_below))
    def _():
        signal(relay.at[0], above)

    @pl.when(jnp.logical_not(has_above))
    def _():
        signal(relay.at[1], below)

    def everyone():
        @pl.when(has_above)
        def _():
            pl.semaphore_wait(relay.at[1], 1)

        @pl.when(has_above & has_below)
        def _():
            signal(relay.at[1], below)

        @pl.when(has_below)
        def _():
            pl.semaphore_wait(relay.at[0], 1)

        @pl.when(has_below & has_above)
        def _():
            signal(relay.at[0], above)

        signal(relay.at[2], across)

    half = part.shape[0] // 2
    chunk = half // mates
    mine = pl.ds(parity * half, half)
    his = pl.ds((1 - parity) * half, half)

    def piece(idx):
        return pl.ds(pl.multiple_of(parity * half + idx * chunk, 8), chunk)

    own = piece(h)

    def g_pair():
        return push(part.at[his], pair_in, g_send.at[0], g_recv.at[0], partner)

    def g_ring(k):
        return push(part.at[piece(mate(k))], ring_in.at[k], g_send.at[k],
                    g_recv.at[k], at(mate(k), c))

    def g_cross():
        return push(gram.at[own], gram.at[own], g_send.at[mates], g_recv.at[mates], across)

    def g_gather(k, idx):
        return push(gram.at[piece(idx)], gram.at[piece(idx)], g_send.at[mates + k],
                    g_recv.at[mates + k], at(mate(k), c))

    def g_half(rows):
        return push(gram.at[rows], gram.at[rows], g_send.at[2 * mates],
                    g_recv.at[2 * mates], partner)

    first_owner = mates // 4
    owners = range(first_owner, mates - first_owner)
    split = mates // 2
    rows_chunk = size // len(owners)
    is_owner = (h >= first_owner) & (h < mates - first_owner)

    def rows_at(offset, count):
        return pl.ds(pl.multiple_of(offset, 8), count)

    y_mine = rows_at(parity * size, size)
    y_his = rows_at((1 - parity) * size, size)

    def y_piece(idx):
        return rows_at(parity * size + (idx - first_owner) * rows_chunk, rows_chunk)

    def y_pair(q):
        if q < 2:
            src, dst = xy.at[q, y_his], xy_pair.at[q]
        else:
            rows = rows_at((1 - parity) * size + (q - 2) * part_rows, part_rows)
            src, dst = xy.at[:, rows], xy_pair.at[:, pl.ds((q - 2) * part_rows, part_rows)]
        return push(src, dst, y_send.at[q % 2], y_recv.at[q % 2], partner)

    def y_merge(q):
        if q < 2:
            xy[q, y_mine] = xy[q, y_mine] + xy_pair[q]
        else:
            rows = rows_at(parity * size + (q - 2) * part_rows, part_rows)
            span = pl.ds((q - 2) * part_rows, part_rows)
            xy[:, rows] = xy[:, rows] + xy_pair[:, span]

    near, far, share, lend, final = (2 + k * mates for k in range(5))

    def y_near(j):
        return push(xy.at[c, y_piece(j)], xy_ring.at[0, h], y_send.at[near + j],
                    y_recv.at[near + h], at(j, c))

    def y_far(j):
        return push(xy.at[other, y_piece(j)], xy_ring.at[1, h], y_send.at[far + j],
                    y_recv.at[far + h], at(j, other))

    def y_arrive(which, j):
        base = (near, far)[which]
        return push(xy_ring.at[which, j], xy_ring.at[which, j], y_send.at[base + j],
                    y_recv.at[base + j], at(j, c))

    def y_share(j):
        view = xy_all.at[c, y_piece(h)]
        return push(view, view, y_send.at[share + j], y_recv.at[share + h], at(j, c))

    def y_lend(j):
        view = xy_all.at[c, y_piece(h)]
        return push(view, view, y_send.at[lend + j], y_recv.at[lend + h], at(j, other))

    def y_result(which, j):
        base, plane = ((share, c), (lend, other))[which]
        view = xy_all.at[plane, y_piece(j)]
        return push(view, view, y_send.at[base + j], y_recv.at[base + j], at(j, plane))

    def y_half(which, plane, rows):
        view = xy_all.at[plane, rows]
        return push(view, view, y_send.at[final + which], y_recv.at[final + which], partner)

    def unless_self(j, step):
        @pl.when(h != j)
        def _():
            step()

    def scatter(q):
        y_pair(q).wait_recv()
        y_merge(q)
        targets = owners if q < 2 else [j for j in owners if (j >= split) == (q == 3)]
        if q != 0:
            for j in targets:
                y_far(j).start()
        if q != 1:
            for j in targets:
                unless_self(j, y_near(j).start)

    def meet(q):
        if q < 2:
            xy[q] = across_rows(xs[:, early], ys[q * size:(q + 1) * size, early])
        else:
            groups = (top, bottom)[q - 2]
            value = across_rows(
                jnp.concatenate([xs[rows, late] for rows in groups], axis=0), ys[:, late])
            for g, rows in enumerate(groups):
                block = value[g * part_rows:(g + 1) * part_rows]
                xy[0, rows] = block[:, :size]
                xy[1, rows] = block[:, size:]
        y_pair(q).start()

    @pl.when(c == 0)
    def _():
        for q in range(2):
            load_copy(q, xs).wait()
            span = early if q == 0 else late
            strip = across_rows(xs[:size, span], xs[:, span])
            rest = across_rows(xs[size:, span], xs[size:, span])
            if q == 0:
                part[:size] = strip[:, :size]
                part[size:2 * size] = strip[:, size:]
                part[2 * size:] = rest
            else:
                part[:size] = part[:size] + strip[:, :size]
                part[size:2 * size] = part[size:2 * size] + strip[:, size:]
                part[2 * size:] = part[2 * size:] + rest
        g_pair().start()

    everyone()

    @pl.when(c == 0)
    def _():
        g_pair().wait_recv()
        part[mine] = part[mine] + pair_in[...]
        for k in range(1, mates):
            g_ring(k).start()
        for k in range(1, mates):
            g_ring(k).wait_recv()
        total = part[own]
        for k in range(1, mates):
            total = total + ring_in[k]
        gram[own] = total
        g_cross().start()
        for q in range(4, 7):
            x_copy(q).start()

    @pl.when(c == 1)
    def _():
        for q in range(2):
            load_copy(q, ys).wait()
        for q in range(2):
            x_copy(q).wait_recv()
        meet(2)
        pl.semaphore_wait(relay.at[2], 1)
        scatter(2)
        g_cross().wait_recv()

    for k in range(1, mates):
        g_gather(k, h).start()

    @pl.when(c == 0)
    def _():
        y_copy(0).wait_recv()
        meet(0)

    @pl.when(c == 1)
    def _():
        for q in range(2, 6):
            x_copy(q).wait_recv()
        meet(3)

    for k in range(1, mates):
        g_gather(k, sender(k)).wait_recv()
    g_half(mine).start()

    @pl.when(c == 0)
    def _():
        scatter(0)

    @pl.when(c == 1)
    def _():
        scatter(3)

    g_half(his).wait_recv()

    eye = (lax.broadcasted_iota(jnp.int32, (size, size), 0)
           == lax.broadcasted_iota(jnp.int32, (size, size), 1)).astype(jnp.float32)
    first[:, :size] = gram[:size]
    first[:, size:2 * size] = gram[size:2 * size]
    first[:, 2 * size:] = eye

    def on_plane(plane, step):
        @pl.when(c == plane)
        def _():
            step()

    def meet_last():
        y_copy(1).wait_recv()
        x_copy(7).start()
        meet(1)

    def scatter_last():
        pl.semaphore_wait(relay.at[2], 1)
        scatter(1)
        for q in range(8, 10):
            x_copy(q).start()

    def gather():
        @pl.when(is_owner)
        def _():
            for j in range(mates):
                unless_self(j, y_arrive(0, j).wait_recv)
            for j in range(mates):
                y_arrive(1, j).wait_recv()
            total = xy[c, y_piece(h)]
            for k in range(1, mates):
                total = total + xy_ring[0, mate(k)]
            for j in range(mates):
                total = total + xy_ring[1, j]
            xy_all[c, y_piece(h)] = total
            for j in range(mates):
                unless_self(j, y_share(j).start)
            for j in range(mates):
                y_lend(j).start()

        @pl.when(c == 0)
        def _():
            x_copy(10).start()

    eliminate(first, {
        1: lambda: on_plane(0, meet_last),
        3: lambda: on_plane(0, scatter_last),
    })

    upper = first[:, size:2 * size]
    cross = contract(upper, first[:, size:], ((0,), (0,)))
    second[:, :size] = gram[2 * size:] - cross[:, :size]
    second[:, size:2 * size] = -cross[:, size:]
    second[:, 2 * size:] = eye
    eliminate(second, {
        1: lambda: on_plane(1, gather),
        4: lambda: on_plane(0, gather),
    })

    inverse[:size, :size] = first[:, 2 * size:]
    inverse[:size, size:] = jnp.zeros((size, size), jnp.float32)
    inverse[size:] = second[:, size:]
    power[...] = contract(inverse[...], inverse[...], ((0,), (0,)))
    own_rows = pl.ds(pl.multiple_of(c * size, size), size)

    def products(lo, count):
        span = pl.ds(lo * eighth, count * eighth)
        q_ref[:, span] = product(inverse[own_rows], xs[:, span]) * scaling
        z_ref[:, span] = product(power[...], xs[:, span])

    keep = (lax.broadcasted_iota(jnp.int32, (size, size), 0)
            <= lax.broadcasted_iota(jnp.int32, (size, size), 1))

    def trail(lo, count):
        span = cols(lo, count)
        tail_ref[:, span] = ys[own_rows, span] - contract(
            xy_all[c], z_ref[:, span], ((0,), (0,)))

    @pl.when(c == 0)
    def _():
        tri_ref[:, :size] = jnp.where(keep, first[:, :size], 0.0) / scaling
        tri_ref[:, size:2 * size] = first[:, size:2 * size] / scaling
        y_copy(2).wait_recv()

    @pl.when(c == 1)
    def _():
        tri_ref[:, :size] = jnp.zeros((size, size), jnp.float32)
        tri_ref[:, size:2 * size] = jnp.where(keep, second[:, :size], 0.0) / scaling
        x_copy(6).wait_recv()

    inv_ref[...] = inverse[own_rows]
    products(4, 4)
    products(0, 1)

    @pl.when(c == 1)
    def _():
        for q in range(7, 10):
            x_copy(q).wait_recv()

    products(1, 2)

    @pl.when(c == 0)
    def _():
        products(3, 1)
        for q in range(10):
            x_copy(q).wait_send()
        g_pair().wait_send()
        for k in range(1, mates):
            g_ring(k).wait_send()
        g_cross().wait_send()
        for q in range(2):
            y_pair(q).wait_send()

    @pl.when(c == 1)
    def _():
        for q in range(len(y_views)):
            y_copy(q).wait_send()
        for q in range(2, 4):
            y_pair(q).wait_send()

    for k in range(1, mates):
        g_gather(k, h).wait_send()
    g_half(mine).wait_send()
    for j in owners:
        unless_self(j, y_near(j).wait_send)
        y_far(j).wait_send()

    for j in owners:
        unless_self(j, y_result(0, j).wait_recv)
    y_half(0, c, y_mine).start()
    for j in owners:
        y_result(1, j).wait_recv()
    y_half(1, other, y_mine).start()
    y_half(0, c, y_his).wait_recv()
    trail(4, 4)
    trail(0, 3)
    sum_ref[c] = xy_all[c]

    @pl.when(is_owner)
    def _():
        for j in range(mates):
            unless_self(j, y_share(j).wait_send)
            y_lend(j).wait_send()

    @pl.when(c == 1)
    def _():
        x_copy(10).wait_recv()
        products(3, 1)

    @pl.when(c == 0)
    def _():
        x_copy(10).wait_send()

    trail(3, 1)
    y_half(1, other, y_his).wait_recv()
    sum_ref[other] = xy_all[other]
    y_half(0, c, y_mine).wait_send()
    y_half(1, other, y_mine).wait_send()


def finish_kernel(scaling, q_in, tail_in, tri_in, inv_ref, sum_ref,
                  ortho_ref, tri_ref, trail_ref, right, sems):
    size = tri_in.shape[0]

    def out(k, src, dst):
        return pltpu.make_async_copy(src, dst, sems.at[k])

    copies = [
        out(0, q_in, ortho_ref),
        out(1, tail_in, trail_ref),
        out(2, tri_in, tri_ref.at[:, :2 * size]),
        out(3, right, tri_ref.at[:, 2 * size:]),
    ]
    for copy in copies[:3]:
        copy.start()
    right[:, :size] = product(inv_ref[...], sum_ref[0]) / scaling
    right[:, size:] = product(inv_ref[...], sum_ref[1]) / scaling
    copies[3].start()
    for copy in copies:
        copy.wait()


def fused(columns):
    row_count = lax.axis_size("rows")
    width = columns.shape[1]
    scaling = math.sqrt(width * row_count)
    size = PANEL
    mates = row_count // 2
    f32 = jnp.float32
    vmem = pl.BlockSpec(memory_space=pltpu.VMEM)
    ortho = jax.ShapeDtypeStruct((size, width), f32)
    triangle = jax.ShapeDtypeStruct((size, 4 * size), f32)
    trailing = ortho
    middle = pl.pallas_call(
        functools.partial(kernel, row_count, scaling),
        out_shape=(
            ortho,
            trailing,
            jax.ShapeDtypeStruct((size, 2 * size), f32),
            jax.ShapeDtypeStruct((size, 2 * size), f32),
            jax.ShapeDtypeStruct((2, 2 * size, size), f32),
        ),
        in_specs=[pl.BlockSpec(memory_space=pltpu.HBM)],
        out_specs=(vmem,) * 5,
        scratch_shapes=[
            pltpu.VMEM((2 * size, width), f32),
            pltpu.VMEM((2 * size, width), f32),
            pltpu.VMEM((3 * size, size), f32),
            pltpu.VMEM((3 * size, size), f32),
            pltpu.VMEM((3 * size // 2, size), f32),
            pltpu.VMEM((mates, 3 * size // row_count, size), f32),
            pltpu.VMEM((size, 3 * size), f32),
            pltpu.VMEM((size, 3 * size), f32),
            pltpu.VMEM((2 * size, 2 * size), f32),
            pltpu.VMEM((2 * size, 2 * size), f32),
            pltpu.VMEM((2 * size, width), f32),
            pltpu.VMEM((2, 2 * size, size), f32),
            pltpu.VMEM((2, size, size), f32),
            pltpu.VMEM((2, mates, size // (mates // 2), size), f32),
            pltpu.VMEM((2, 2 * size, size), f32),
            pltpu.SemaphoreType.DMA((2,)),
            pltpu.SemaphoreType.DMA((11,)),
            pltpu.SemaphoreType.DMA((11,)),
            pltpu.SemaphoreType.DMA((2 * mates + 1,)),
            pltpu.SemaphoreType.DMA((2 * mates + 1,)),
            pltpu.SemaphoreType.DMA((4 * mates + 4,)),
            pltpu.SemaphoreType.DMA((4 * mates + 4,)),
            pltpu.SemaphoreType.REGULAR((3,)),
        ],
        compiler_params=pltpu.CompilerParams(
            collective_id=0, has_side_effects=True, vmem_limit_bytes=VMEM_BYTES),
    )(pltpu.with_memory_space_constraint(columns, pltpu.HBM))
    return pl.pallas_call(
        functools.partial(finish_kernel, scaling),
        out_shape=(ortho, triangle, trailing),
        in_specs=[vmem] * 5,
        out_specs=(pl.BlockSpec(memory_space=pltpu.HBM),) * 3,
        scratch_shapes=[
            pltpu.VMEM((size, 2 * size), f32),
            pltpu.SemaphoreType.DMA((4,)),
        ],
        compiler_params=pltpu.CompilerParams(vmem_limit_bytes=VMEM_BYTES),
    )(*middle)


def inverse_lower(lower):
    identity = jnp.eye(lower.shape[0], dtype=lower.dtype)
    return lax.linalg.triangular_solve(lower, identity, left_side=True, lower=True)


def summed(partial_term):
    return lax.psum(partial_term, "rows")


def general(columns):
    col_count = lax.axis_size("cols")
    col_index = lax.axis_index("cols")
    scaling = math.sqrt(columns.shape[1] * lax.axis_size("rows"))
    local_rows = lax.all_gather(columns, "cols", axis=0, tiled=True)
    panel_count = 2 * PANEL
    leading = local_rows[:panel_count]
    gram_strip = summed(product(leading, local_rows.T))
    lower_both = jnp.linalg.cholesky(gram_strip[:, :panel_count])
    inverse_both = inverse_lower(lower_both)
    orthonormal = product(inverse_both, leading)
    coupling = product(inverse_both, gram_strip[:, panel_count:])
    trailing = local_rows[panel_count:] - product(coupling.T, orthonormal)
    triangle = jnp.concatenate([lower_both.T, coupling], axis=1)
    orthonormal = orthonormal * scaling
    triangle = triangle / scaling

    def own(array):
        count = array.shape[0] // col_count
        return lax.dynamic_slice_in_dim(array, col_index * count, count, 0)

    return (own(orthonormal), own(triangle), own(trailing))


def shards(columns):
    rows = lax.axis_size("rows")
    paired = lax.axis_size("cols") == 2 and columns.shape[0] == 2 * PANEL and columns.shape[1] % (8 * PANEL) == 0
    if paired and rows % 8 == 0 and (2 * PANEL) % (8 * rows) == 0 and (3 * PANEL) % (8 * rows) == 0:
        return fused(columns)
    return general(columns)


def solution(mesh):
    placed = (P("cols", "rows"),)
    return jax.shard_map(
        shards,
        mesh=mesh,
        in_specs=placed,
        out_specs=(P("cols", "rows"), P("cols", None), P("cols", "rows")),
        check_vma=False,
    )
```

```python
import functools
import math

import jax
import jax.numpy as jnp
from jax import lax
from jax.experimental import pallas as pl
from jax.experimental.pallas import tpu as pltpu
from jax.sharding import PartitionSpec as P

PANEL = 128
STRIP = 16
VMEM_BYTES = 20 * 2**20
MESH = pl.DeviceIdType.MESH

precise = lax.Precision.HIGHEST


def product(left, right):
    return jnp.dot(left, right, precision=precise, preferred_element_type=jnp.float32)


def contract(left, right, dims):
    return lax.dot_general(
        left, right, (dims, ((), ())), precision=precise, preferred_element_type=jnp.float32
    )


def across_rows(left, right):
    return contract(left, right, ((1,), (1,)))


def pieces(value):
    first = value.astype(jnp.bfloat16)
    rest = value - first.astype(jnp.float32)
    second = rest.astype(jnp.bfloat16)
    third = (rest - second.astype(jnp.float32)).astype(jnp.bfloat16)
    return first, second, third


def strip_update(left, right, after):
    a, b, c = pieces(left)
    d, e, f = pieces(right)
    lhs = jnp.concatenate([a, a, b, a, c, b], axis=0)
    rhs = jnp.concatenate([d, e, d, f, d, e], axis=0)
    return jnp.dot(lhs.T[after:], rhs, preferred_element_type=jnp.float32)


def root_inverse(value):
    guess = lax.rsqrt(value)
    return guess * (1.5 - (0.5 * value) * guess * guess)


def eliminate(ref, hooks):
    size = ref.shape[0]
    lanes = size
    parts = ref.shape[1] // lanes
    below = lax.broadcasted_iota(jnp.int32, (STRIP, lanes), 0)
    for s in range(size // STRIP):
        at = s * STRIP
        rows = [ref[at:at + STRIP, q * lanes:(q + 1) * lanes] for q in range(parts)]
        cols = [
            jnp.broadcast_to(rows[0][:, at + j:at + j + 1], (STRIP, lanes))
            for j in range(STRIP)
        ]
        scales = [lax.rsqrt(cols[i][i:i + 1]) for i in range(0, STRIP, 2)]
        for i in range(0, STRIP, 2):
            scale = scales[i // 2]
            corner = cols[i][i:i + 1]
            edge = cols[i][i + 1:i + 2]
            unit = corner * scale * scale
            minor = unit * cols[i + 1][i + 1:i + 2] - edge * scale * scale * edge
            inv = root_inverse(corner)
            inv_next = root_inverse(minor) * (unit * root_inverse(unit))
            col = cols[i] * inv
            col_next = (cols[i + 1] - col * col[i + 1:i + 2]) * inv_next
            coef = jnp.where(below > i, col, 0.0)
            coef_next = jnp.where(below > i + 1, col_next, 0.0)
            for j in range(i + 2, STRIP):
                cols[j] = cols[j] - coef * col[j:j + 1] - coef_next * col_next[j:j + 1]
            for q in range(parts):
                row = rows[q][i:i + 1] * inv
                rest = rows[q] - coef * row
                row_next = rest[i + 1:i + 2] * inv_next
                rest = jnp.where(below == i + 1, row_next, rest - coef_next * row_next)
                rows[q] = jnp.where(below == i, row, rest)
        for q in range(parts):
            ref[at:at + STRIP, q * lanes:(q + 1) * lanes] = rows[q]
        after = at + STRIP
        if after < size:
            update = strip_update(rows[0], jnp.concatenate(rows, axis=1), after)
            ref[after:, :] = ref[after:, :] - update
        if s in hooks:
            hooks[s]()


def kernel(row_count, scaling, x_ref, q_ref, tail_ref, tri_ref, inv_ref, sum_ref,
           xs, ys, part, gram, pair_in, ring_in, first, second, inverse, power, z_ref,
           xy, xy_pair, xy_ring, xy_all, load, x_send, x_recv, g_send, g_recv,
           y_send, y_recv, relay):
    r = lax.axis_index("rows")
    c = lax.axis_index("cols")
    other = 1 - c
    parity = lax.rem(r, 2)
    h = r // 2
    mates = row_count // 2
    line = mates // 2
    place = h // 2
    partner = (r + 1 - 2 * parity, c)
    across = (r, other)
    side = ((h + 1 - 2 * lax.rem(h, 2)) * 2 + parity, c)
    above = (r + 4, c)
    below = (r - 4, c)
    has_above = place < line - 1
    has_below = place > 0
    size = PANEL
    width = xs.shape[1]
    half_width = width // 2
    eighth = width // 8

    def mate(k):
        return lax.rem(h + k, mates)

    def at(idx, plane):
        return (idx * 2 + parity, plane)

    def push(src, dst, send_sem, recv_sem, target):
        return pltpu.make_async_remote_copy(
            src_ref=src, dst_ref=dst, send_sem=send_sem, recv_sem=recv_sem,
            device_id=target, device_id_type=MESH)

    def signal(sem, target):
        pl.semaphore_signal(sem, inc=1, device_id=target, device_id_type=MESH)

    barrier = pltpu.get_barrier_semaphore()
    for target in (across, partner, side):
        signal(barrier, target)

    @pl.when(has_above)
    def _():
        signal(barrier, above)

    @pl.when(has_below)
    def _():
        signal(barrier, below)

    early = pl.ds(0, half_width)
    late = pl.ds(half_width, half_width)

    def load_copy(q, dst):
        span = early if q == 0 else late
        return pltpu.make_async_copy(x_ref.at[:, span], dst.at[:, span], load.at[q])

    @pl.when(c == 0)
    def _():
        for q in range(2):
            load_copy(q, xs).start()

    @pl.when(c == 1)
    def _():
        for q in range(2):
            load_copy(q, ys).start()

    pl.semaphore_wait(barrier, 3 + has_above.astype(jnp.int32) + has_below.astype(jnp.int32))

    part_rows = size // 2
    top = [pl.ds(q * size, part_rows) for q in range(2)]
    bottom = [pl.ds(q * size + part_rows, part_rows) for q in range(2)]
    every = pl.ds(0, 2 * size)

    def cols(lo, count):
        return pl.ds(lo * eighth, count * eighth)

    x_views = (
        [(rows, late) for rows in top]
        + [(rows, cols(4, 2)) for rows in bottom]
        + [(rows, cols(6, 2)) for rows in bottom]
        + [(every, cols(0, 1)), (pl.ds(0, size), cols(1, 1)), (pl.ds(size, size), cols(1, 1)),
           (every, cols(2, 1)), (every, cols(3, 1))]
    )
    y_views = [(pl.ds(0, size), early), (pl.ds(size, size), early), (pl.ds(0, size), late)]

    x_group = (0, 0, 1, 1, 1, 1, 2, 3, 3, 3, 4)

    def x_copy(q):
        return push(x_ref.at[x_views[q]], xs.at[x_views[q]], x_send.at[0],
                    x_recv.at[x_group[q]], across)

    def y_copy(q):
        return push(x_ref.at[y_views[q]], ys.at[y_views[q]], x_send.at[0], x_recv.at[q], across)

    def bulk(ref, send_sem, recv_sem):
        return push(ref, ref, send_sem, recv_sem, across)

    x_sizes = ((size, late), (size, late), (2 * size, cols(0, 1)), (2 * size, cols(1, 2)),
               (2 * size, cols(3, 1)))

    def x_group_wait(g):
        rows, span = x_sizes[g]
        bulk(xs.at[pl.ds(0, rows), span], x_send.at[0], x_recv.at[g]).wait_recv()

    def bulk_sent():
        @pl.when(c == 0)
        def _():
            bulk(xs, x_send.at[0], x_recv.at[0]).wait_send()

        @pl.when(c == 1)
        def _():
            bulk(ys.at[pl.ds(0, 3 * size // 2)], x_send.at[0], x_recv.at[0]).wait_send()

    @pl.when(c == 0)
    def _():
        for q in range(4):
            x_copy(q).start()

    @pl.when(c == 1)
    def _():
        for q in range(3):
            y_copy(q).start()

    up_next = has_below & has_above
    up_waits = place > 1
    down_next = has_above & has_below
    down_waits = place < line - 2

    @pl.when(up_next & jnp.logical_not(up_waits))
    def _():
        signal(relay.at[0], above)

    @pl.when(down_next & jnp.logical_not(down_waits))
    def _():
        signal(relay.at[1], below)

    def everyone():
        @pl.when(up_waits)
        def _():
            pl.semaphore_wait(relay.at[0], 1)

        @pl.when(up_waits & up_next)
        def _():
            signal(relay.at[0], above)

        @pl.when(down_waits)
        def _():
            pl.semaphore_wait(relay.at[1], 1)

        @pl.when(down_waits & down_next)
        def _():
            signal(relay.at[1], below)

        signal(relay.at[3], side)
        pl.semaphore_wait(relay.at[3], 1)
        signal(relay.at[2], across)

    half = part.shape[0] // 2
    chunk = half // mates
    mine = pl.ds(parity * half, half)
    his = pl.ds((1 - parity) * half, half)

    def piece(idx):
        return pl.ds(pl.multiple_of(parity * half + idx * chunk, 8), chunk)

    own = piece(h)

    def g_pair():
        return push(part.at[his], pair_in, g_send.at[0], g_recv.at[0], partner)

    def g_ring(k):
        return push(part.at[piece(mate(k))], ring_in.at[k], g_send.at[0],
                    g_recv.at[1], at(mate(k), c))

    def g_cross():
        return push(gram.at[own], gram.at[own], g_send.at[0], g_recv.at[2], across)

    def g_gather(k):
        return push(gram.at[own], gram.at[own], g_send.at[1], g_recv.at[3], at(mate(k), c))

    def g_half(rows):
        return push(gram.at[rows], gram.at[rows], g_send.at[1], g_recv.at[4], partner)

    def amount(ref, send_sem, recv_sem):
        return push(ref, ref, send_sem, recv_sem, partner)

    first_owner = mates // 4
    owners = range(first_owner, mates - first_owner)
    split = mates // 2
    rows_chunk = size // len(owners)
    is_owner = (h >= first_owner) & (h < mates - first_owner)

    def rows_at(offset, count):
        return pl.ds(pl.multiple_of(offset, 8), count)

    y_mine = rows_at(parity * size, size)
    y_his = rows_at((1 - parity) * size, size)

    def y_piece(idx):
        return rows_at(parity * size + (idx - first_owner) * rows_chunk, rows_chunk)

    def y_pair(q):
        if q < 2:
            src, dst = xy.at[q, y_his], xy_pair.at[q]
        else:
            rows = rows_at((1 - parity) * size + (q - 2) * part_rows, part_rows)
            src, dst = xy.at[:, rows], xy_pair.at[:, pl.ds((q - 2) * part_rows, part_rows)]
        return push(src, dst, y_send.at[0], y_recv.at[q % 2], partner)

    def y_merge(q):
        if q < 2:
            xy[q, y_mine] = xy[q, y_mine] + xy_pair[q]
        else:
            rows = rows_at(parity * size + (q - 2) * part_rows, part_rows)
            span = pl.ds((q - 2) * part_rows, part_rows)
            xy[:, rows] = xy[:, rows] + xy_pair[:, span]

    near, far, share, lend, final = range(2, 7)

    def y_near(j):
        return push(xy.at[c, y_piece(j)], xy_ring.at[0, h], y_send.at[1],
                    y_recv.at[near], at(j, c))

    def y_far(j):
        return push(xy.at[other, y_piece(j)], xy_ring.at[1, h], y_send.at[0],
                    y_recv.at[far], at(j, other))

    def y_share(j):
        view = xy_all.at[c, y_piece(h)]
        return push(view, view, y_send.at[2], y_recv.at[share], at(j, c))

    def y_lend(j):
        view = xy_all.at[c, y_piece(h)]
        return push(view, view, y_send.at[3], y_recv.at[lend], at(j, other))

    def y_half(which, plane, rows):
        view = xy_all.at[plane, rows]
        return push(view, view, y_send.at[4], y_recv.at[final + which], partner)

    def by_role(count, step):
        @pl.when(is_owner)
        def _():
            step(count - 1)

        @pl.when(jnp.logical_not(is_owner))
        def _():
            step(count)

    def unless_self(j, step):
        @pl.when(h != j)
        def _():
            step()

    def scatter(q):
        y_pair(q).wait_recv()
        y_merge(q)
        targets = owners if q < 2 else [j for j in owners if (j >= split) == (q == 3)]
        if q != 0:
            for j in targets:
                y_far(j).start()
        if q != 1:
            for j in targets:
                unless_self(j, y_near(j).start)

    def meet(q):
        if q < 2:
            xy[q] = across_rows(xs[:, early], ys[q * size:(q + 1) * size, early])
        else:
            groups = (top, bottom)[q - 2]
            value = across_rows(
                jnp.concatenate([xs[rows, late] for rows in groups], axis=0), ys[:, late])
            for g, rows in enumerate(groups):
                block = value[g * part_rows:(g + 1) * part_rows]
                xy[0, rows] = block[:, :size]
                xy[1, rows] = block[:, size:]
        y_pair(q).start()

    @pl.when(c == 0)
    def _():
        for q in range(2):
            load_copy(q, xs).wait()
            span = early if q == 0 else late
            strip = across_rows(xs[:size, span], xs[:, span])
            rest = across_rows(xs[size:, span], xs[size:, span])
            if q == 0:
                part[:size] = strip[:, :size]
                part[size:2 * size] = strip[:, size:]
                part[2 * size:] = rest
            else:
                part[:size] = part[:size] + strip[:, :size]
                part[size:2 * size] = part[size:2 * size] + strip[:, size:]
                part[2 * size:] = part[2 * size:] + rest
        g_pair().start()

    everyone()

    @pl.when(c == 0)
    def _():
        g_pair().wait_recv()
        part[mine] = part[mine] + pair_in[...]
        for k in range(1, mates):
            g_ring(k).start()
        amount(ring_in.at[pl.ds(1, mates - 1)], g_send.at[0], g_recv.at[1]).wait_recv()
        total = part[own]
        for k in range(1, mates):
            total = total + ring_in[k]
        gram[own] = total
        g_cross().start()
        for q in range(4, 7):
            x_copy(q).start()

    @pl.when(c == 1)
    def _():
        for q in range(2):
            load_copy(q, ys).wait()
        x_group_wait(0)
        meet(2)
        pl.semaphore_wait(relay.at[2], 1)
        scatter(2)
        g_cross().wait_recv()

    for k in range(1, mates):
        g_gather(k).start()

    @pl.when(c == 0)
    def _():
        y_copy(0).wait_recv()
        meet(0)

    @pl.when(c == 1)
    def _():
        x_group_wait(1)
        meet(3)
        scatter(3)

    amount(gram.at[pl.ds(0, (mates - 1) * chunk)], g_send.at[1], g_recv.at[3]).wait_recv()
    g_half(mine).start()

    @pl.when(c == 0)
    def _():
        scatter(0)

    g_half(his).wait_recv()

    eye = (lax.broadcasted_iota(jnp.int32, (size, size), 0)
           == lax.broadcasted_iota(jnp.int32, (size, size), 1)).astype(jnp.float32)
    first[:, :size] = gram[:size]
    first[:, size:2 * size] = gram[size:2 * size]
    first[:, 2 * size:] = eye

    def on_plane(plane, step):
        @pl.when(c == plane)
        def _():
            step()

    def meet_last():
        y_copy(1).wait_recv()
        x_copy(7).start()
        meet(1)

    def scatter_last():
        pl.semaphore_wait(relay.at[2], 1)
        scatter(1)
        for q in range(8, 10):
            x_copy(q).start()

    def gather():
        @pl.when(is_owner)
        def _():
            amount(xy_ring.at[0, pl.ds(0, mates - 1)], y_send.at[1], y_recv.at[near]).wait_recv()
            amount(xy_ring.at[1], y_send.at[0], y_recv.at[far]).wait_recv()
            total = xy[c, y_piece(h)]
            for k in range(1, mates):
                total = total + xy_ring[0, mate(k)]
            for j in range(mates):
                total = total + xy_ring[1, j]
            xy_all[c, y_piece(h)] = total
            for j in range(mates):
                unless_self(j, y_share(j).start)
            for j in range(mates):
                y_lend(j).start()

        @pl.when(c == 0)
        def _():
            x_copy(10).start()

    eliminate(first, {
        0: lambda: on_plane(0, meet_last),
        2: lambda: on_plane(0, scatter_last),
    })

    upper = first[:, size:2 * size]
    cross = contract(upper, first[:, size:], ((0,), (0,)))
    second[:, :size] = gram[2 * size:] - cross[:, :size]
    second[:, size:2 * size] = -cross[:, size:]
    second[:, 2 * size:] = eye
    eliminate(second, {
        1: lambda: on_plane(1, gather),
        3: lambda: on_plane(0, gather),
    })

    inverse[:size, :size] = first[:, 2 * size:]
    inverse[:size, size:] = jnp.zeros((size, size), jnp.float32)
    inverse[size:] = second[:, size:]
    power[...] = contract(inverse[...], inverse[...], ((0,), (0,)))
    own_rows = pl.ds(pl.multiple_of(c * size, size), size)

    def products(lo, count):
        span = pl.ds(lo * eighth, count * eighth)
        q_ref[:, span] = product(inverse[own_rows], xs[:, span]) * scaling
        z_ref[:, span] = product(power[...], xs[:, span])

    keep = (lax.broadcasted_iota(jnp.int32, (size, size), 0)
            <= lax.broadcasted_iota(jnp.int32, (size, size), 1))

    def trail(lo, count):
        span = cols(lo, count)
        tail_ref[:, span] = ys[own_rows, span] - contract(
            xy_all[c], z_ref[:, span], ((0,), (0,)))

    @pl.when(c == 0)
    def _():
        tri_ref[:, :size] = jnp.where(keep, first[:, :size], 0.0) / scaling
        tri_ref[:, size:2 * size] = first[:, size:2 * size] / scaling
        y_copy(2).wait_recv()

    @pl.when(c == 1)
    def _():
        tri_ref[:, :size] = jnp.zeros((size, size), jnp.float32)
        tri_ref[:, size:2 * size] = jnp.where(keep, second[:, :size], 0.0) / scaling
        x_group_wait(2)

    inv_ref[...] = inverse[own_rows]
    products(4, 4)
    products(0, 1)

    @pl.when(c == 1)
    def _():
        x_group_wait(3)

    products(1, 2)

    @pl.when(c == 0)
    def _():
        products(3, 1)
        amount(part, g_send.at[0], g_recv.at[0]).wait_send()

    amount(gram.at[pl.ds(0, (mates - 1) * chunk + half)], g_send.at[1], g_recv.at[0]).wait_send()
    amount(part, y_send.at[0], y_recv.at[0]).wait_send()

    def rows_of(count):
        return xy_all.at[0, pl.ds(0, count * rows_chunk)]

    by_role(len(owners), lambda n: amount(
        rows_of(n), y_send.at[1], y_recv.at[0]).wait_send())
    by_role(len(owners), lambda n: amount(
        rows_of(n), y_send.at[1], y_recv.at[share]).wait_recv())
    y_half(0, c, y_mine).start()
    amount(rows_of(len(owners)), y_send.at[1], y_recv.at[lend]).wait_recv()
    y_half(1, other, y_mine).start()
    y_half(0, c, y_his).wait_recv()
    trail(4, 4)
    trail(0, 3)
    sum_ref[c] = xy_all[c]

    @pl.when(is_owner)
    def _():
        amount(rows_of(mates - 1), y_send.at[2], y_recv.at[0]).wait_send()
        amount(rows_of(mates), y_send.at[3], y_recv.at[0]).wait_send()

    @pl.when(c == 1)
    def _():
        x_group_wait(4)
        products(3, 1)

    bulk_sent()
    trail(3, 1)
    y_half(1, other, y_his).wait_recv()
    sum_ref[other] = xy_all[other]
    amount(xy_pair, y_send.at[4], y_recv.at[0]).wait_send()


def finish_kernel(scaling, q_in, tail_in, tri_in, inv_ref, sum_ref,
                  ortho_ref, tri_ref, trail_ref, right, sems):
    size = tri_in.shape[0]

    def out(k, src, dst):
        return pltpu.make_async_copy(src, dst, sems.at[k])

    copies = [
        out(0, q_in, ortho_ref),
        out(1, tail_in, trail_ref),
        out(2, tri_in, tri_ref.at[:, :2 * size]),
        out(3, right, tri_ref.at[:, 2 * size:]),
    ]
    for copy in copies[:3]:
        copy.start()
    right[:, :size] = product(inv_ref[...], sum_ref[0]) / scaling
    right[:, size:] = product(inv_ref[...], sum_ref[1]) / scaling
    copies[3].start()
    for copy in copies:
        copy.wait()


def fused(columns):
    row_count = lax.axis_size("rows")
    width = columns.shape[1]
    scaling = math.sqrt(width * row_count)
    size = PANEL
    mates = row_count // 2
    f32 = jnp.float32
    vmem = pl.BlockSpec(memory_space=pltpu.VMEM)
    ortho = jax.ShapeDtypeStruct((size, width), f32)
    triangle = jax.ShapeDtypeStruct((size, 4 * size), f32)
    trailing = ortho
    middle = pl.pallas_call(
        functools.partial(kernel, row_count, scaling),
        out_shape=(
            ortho,
            trailing,
            jax.ShapeDtypeStruct((size, 2 * size), f32),
            jax.ShapeDtypeStruct((size, 2 * size), f32),
            jax.ShapeDtypeStruct((2, 2 * size, size), f32),
        ),
        in_specs=[pl.BlockSpec(memory_space=pltpu.HBM)],
        out_specs=(vmem,) * 5,
        scratch_shapes=[
            pltpu.VMEM((2 * size, width), f32),
            pltpu.VMEM((2 * size, width), f32),
            pltpu.VMEM((3 * size, size), f32),
            pltpu.VMEM((3 * size, size), f32),
            pltpu.VMEM((3 * size // 2, size), f32),
            pltpu.VMEM((mates, 3 * size // row_count, size), f32),
            pltpu.VMEM((size, 3 * size), f32),
            pltpu.VMEM((size, 3 * size), f32),
            pltpu.VMEM((2 * size, 2 * size), f32),
            pltpu.VMEM((2 * size, 2 * size), f32),
            pltpu.VMEM((2 * size, width), f32),
            pltpu.VMEM((2, 2 * size, size), f32),
            pltpu.VMEM((2, size, size), f32),
            pltpu.VMEM((2, mates, size // (mates // 2), size), f32),
            pltpu.VMEM((2, 2 * size, size), f32),
            pltpu.SemaphoreType.DMA((2,)),
            pltpu.SemaphoreType.DMA((1,)),
            pltpu.SemaphoreType.DMA((5,)),
            pltpu.SemaphoreType.DMA((2,)),
            pltpu.SemaphoreType.DMA((5,)),
            pltpu.SemaphoreType.DMA((5,)),
            pltpu.SemaphoreType.DMA((8,)),
            pltpu.SemaphoreType.REGULAR((4,)),
        ],
        compiler_params=pltpu.CompilerParams(
            collective_id=0, has_side_effects=True, vmem_limit_bytes=VMEM_BYTES),
    )(pltpu.with_memory_space_constraint(columns, pltpu.HBM))
    return pl.pallas_call(
        functools.partial(finish_kernel, scaling),
        out_shape=(ortho, triangle, trailing),
        in_specs=[vmem] * 5,
        out_specs=(pl.BlockSpec(memory_space=pltpu.HBM),) * 3,
        scratch_shapes=[
            pltpu.VMEM((size, 2 * size), f32),
            pltpu.SemaphoreType.DMA((4,)),
        ],
        compiler_params=pltpu.CompilerParams(vmem_limit_bytes=VMEM_BYTES),
    )(*middle)


def inverse_lower(lower):
    identity = jnp.eye(lower.shape[0], dtype=lower.dtype)
    return lax.linalg.triangular_solve(lower, identity, left_side=True, lower=True)


def summed(partial_term):
    return lax.psum(partial_term, "rows")


def general(columns):
    col_count = lax.axis_size("cols")
    col_index = lax.axis_index("cols")
    scaling = math.sqrt(columns.shape[1] * lax.axis_size("rows"))
    local_rows = lax.all_gather(columns, "cols", axis=0, tiled=True)
    panel_count = 2 * PANEL
    leading = local_rows[:panel_count]
    gram_strip = summed(product(leading, local_rows.T))
    lower_both = jnp.linalg.cholesky(gram_strip[:, :panel_count])
    inverse_both = inverse_lower(lower_both)
    orthonormal = product(inverse_both, leading)
    coupling = product(inverse_both, gram_strip[:, panel_count:])
    trailing = local_rows[panel_count:] - product(coupling.T, orthonormal)
    triangle = jnp.concatenate([lower_both.T, coupling], axis=1)
    orthonormal = orthonormal * scaling
    triangle = triangle / scaling

    def own(array):
        count = array.shape[0] // col_count
        return lax.dynamic_slice_in_dim(array, col_index * count, count, 0)

    return (own(orthonormal), own(triangle), own(trailing))


def shards(columns):
    rows = lax.axis_size("rows")
    paired = lax.axis_size("cols") == 2 and columns.shape[0] == 2 * PANEL and columns.shape[1] % (8 * PANEL) == 0
    if paired and rows % 8 == 0 and (2 * PANEL) % (8 * rows) == 0 and (3 * PANEL) % (8 * rows) == 0:
        return fused(columns)
    return general(columns)


def solution(mesh):
    placed = (P("cols", "rows"),)
    return jax.shard_map(
        shards,
        mesh=mesh,
        in_specs=placed,
        out_specs=(P("cols", "rows"), P("cols", None), P("cols", "rows")),
        check_vma=False,
    )
```

```python
import functools
import math

import jax
import jax.numpy as jnp
from jax import lax
from jax.experimental import pallas as pl
from jax.experimental.pallas import tpu as pltpu
from jax.sharding import PartitionSpec as P

PANEL = 128
STRIP = 16
VMEM_BYTES = 20 * 2**20
MESH = pl.DeviceIdType.MESH

precise = lax.Precision.HIGHEST


def product(left, right):
    return jnp.dot(left, right, precision=precise, preferred_element_type=jnp.float32)


def contract(left, right, dims):
    return lax.dot_general(
        left, right, (dims, ((), ())), precision=precise, preferred_element_type=jnp.float32
    )


def across_rows(left, right):
    return contract(left, right, ((1,), (1,)))


def pieces(value):
    first = value.astype(jnp.bfloat16)
    rest = value - first.astype(jnp.float32)
    second = rest.astype(jnp.bfloat16)
    third = (rest - second.astype(jnp.float32)).astype(jnp.bfloat16)
    return first, second, third


def strip_update(left, right, after):
    a, b, c = pieces(left)
    d, e, f = pieces(right)
    lhs = jnp.concatenate([a, a, b, a, c, b], axis=0)
    rhs = jnp.concatenate([d, e, d, f, d, e], axis=0)
    return jnp.dot(lhs.T[after:], rhs, preferred_element_type=jnp.float32)


def root_inverse(value):
    guess = lax.rsqrt(value)
    return guess * (1.5 - (0.5 * value) * guess * guess)


def eliminate(ref, hooks):
    size = ref.shape[0]
    lanes = size
    parts = ref.shape[1] // lanes
    below = lax.broadcasted_iota(jnp.int32, (STRIP, lanes), 0)
    for s in range(size // STRIP):
        at = s * STRIP
        rows = [ref[at:at + STRIP, q * lanes:(q + 1) * lanes] for q in range(parts)]
        cols = [
            jnp.broadcast_to(rows[0][:, at + j:at + j + 1], (STRIP, lanes))
            for j in range(STRIP)
        ]
        scales = [lax.rsqrt(cols[i][i:i + 1]) for i in range(0, STRIP, 2)]
        for i in range(0, STRIP, 2):
            scale = scales[i // 2]
            corner = cols[i][i:i + 1]
            edge = cols[i][i + 1:i + 2]
            unit = corner * scale * scale
            minor = unit * cols[i + 1][i + 1:i + 2] - edge * scale * scale * edge
            inv = root_inverse(corner)
            inv_next = root_inverse(minor) * (unit * root_inverse(unit))
            col = cols[i] * inv
            col_next = (cols[i + 1] - col * col[i + 1:i + 2]) * inv_next
            coef = jnp.where(below > i, col, 0.0)
            coef_next = jnp.where(below > i + 1, col_next, 0.0)
            for j in range(i + 2, STRIP):
                cols[j] = cols[j] - coef * col[j:j + 1] - coef_next * col_next[j:j + 1]
            for q in range(parts):
                row = rows[q][i:i + 1] * inv
                rest = rows[q] - coef * row
                row_next = rest[i + 1:i + 2] * inv_next
                rest = jnp.where(below == i + 1, row_next, rest - coef_next * row_next)
                rows[q] = jnp.where(below == i, row, rest)
        for q in range(parts):
            ref[at:at + STRIP, q * lanes:(q + 1) * lanes] = rows[q]
        after = at + STRIP
        if after < size:
            update = strip_update(rows[0], jnp.concatenate(rows, axis=1), after)
            ref[after:, :] = ref[after:, :] - update
        if s in hooks:
            hooks[s]()


def kernel(row_count, scaling, x_ref, q_ref, tail_ref, tri_ref, inv_ref, sum_ref,
           xs, ys, part, gram, pair_in, ring_in, first, second, inverse, factors, z_ref,
           xy, xy_pair, xy_ring, xy_all, load, x_send, x_recv, g_send, g_recv,
           y_send, y_recv, relay):
    r = lax.axis_index("rows")
    c = lax.axis_index("cols")
    other = 1 - c
    parity = lax.rem(r, 2)
    h = r // 2
    mates = row_count // 2
    line = mates // 2
    place = h // 2
    partner = (r + 1 - 2 * parity, c)
    across = (r, other)
    side = ((h + 1 - 2 * lax.rem(h, 2)) * 2 + parity, c)
    above = (r + 4, c)
    below = (r - 4, c)
    has_above = place < line - 1
    has_below = place > 0
    size = PANEL
    width = xs.shape[1]
    half_width = width // 2
    eighth = width // 8

    def mate(k):
        return lax.rem(h + k, mates)

    def at(idx, plane):
        return (idx * 2 + parity, plane)

    def push(src, dst, send_sem, recv_sem, target):
        return pltpu.make_async_remote_copy(
            src_ref=src, dst_ref=dst, send_sem=send_sem, recv_sem=recv_sem,
            device_id=target, device_id_type=MESH)

    def signal(sem, target):
        pl.semaphore_signal(sem, inc=1, device_id=target, device_id_type=MESH)

    barrier = pltpu.get_barrier_semaphore()
    for target in (across, partner, side):
        signal(barrier, target)

    @pl.when(has_above)
    def _():
        signal(barrier, above)

    @pl.when(has_below)
    def _():
        signal(barrier, below)

    early = pl.ds(0, half_width)
    late = pl.ds(half_width, half_width)

    def load_copy(q, dst):
        span = early if q == 0 else late
        return pltpu.make_async_copy(x_ref.at[:, span], dst.at[:, span], load.at[q])

    @pl.when(c == 0)
    def _():
        for q in range(2):
            load_copy(q, xs).start()

    @pl.when(c == 1)
    def _():
        for q in range(2):
            load_copy(q, ys).start()

    pl.semaphore_wait(barrier, 3 + has_above.astype(jnp.int32) + has_below.astype(jnp.int32))

    part_rows = size // 2
    top = [pl.ds(q * size, part_rows) for q in range(2)]
    bottom = [pl.ds(q * size + part_rows, part_rows) for q in range(2)]
    every = pl.ds(0, 2 * size)

    def cols(lo, count):
        return pl.ds(lo * eighth, count * eighth)

    x_views = (
        [(rows, late) for rows in top]
        + [(rows, late) for rows in bottom]
        + [(every, cols(0, 1)), (pl.ds(0, size), cols(1, 1)), (pl.ds(size, size), cols(1, 1)),
           (every, cols(2, 1)), (every, cols(3, 1))]
    )
    y_views = [(pl.ds(0, size), early), (pl.ds(size, size), early), (pl.ds(0, size), late)]

    x_group = (0, 0, 1, 1, 2, 2, 2, 2, 3)

    def x_copy(q):
        return push(x_ref.at[x_views[q]], xs.at[x_views[q]], x_send.at[0],
                    x_recv.at[x_group[q]], across)

    def y_copy(q):
        return push(x_ref.at[y_views[q]], ys.at[y_views[q]], x_send.at[0], x_recv.at[q], across)

    def bulk(ref, send_sem, recv_sem):
        return push(ref, ref, send_sem, recv_sem, across)

    x_sizes = ((size, late), (size, late), (2 * size, cols(0, 3)),
               (2 * size, cols(3, 1)))

    def x_group_wait(g):
        rows, span = x_sizes[g]
        bulk(xs.at[pl.ds(0, rows), span], x_send.at[0], x_recv.at[g]).wait_recv()

    def bulk_sent():
        @pl.when(c == 0)
        def _():
            bulk(xs, x_send.at[0], x_recv.at[0]).wait_send()

        @pl.when(c == 1)
        def _():
            bulk(ys.at[pl.ds(0, 3 * size // 2)], x_send.at[0], x_recv.at[0]).wait_send()

    @pl.when(c == 0)
    def _():
        for q in range(5):
            x_copy(q).start()

    @pl.when(c == 1)
    def _():
        for q in range(3):
            y_copy(q).start()

    up_next = has_below & has_above
    up_waits = place > 1
    down_next = has_above & has_below
    down_waits = place < line - 2

    @pl.when(up_next & jnp.logical_not(up_waits))
    def _():
        signal(relay.at[0], above)

    @pl.when(down_next & jnp.logical_not(down_waits))
    def _():
        signal(relay.at[1], below)

    def everyone():
        @pl.when(up_waits)
        def _():
            pl.semaphore_wait(relay.at[0], 1)

        @pl.when(up_waits & up_next)
        def _():
            signal(relay.at[0], above)

        @pl.when(down_waits)
        def _():
            pl.semaphore_wait(relay.at[1], 1)

        @pl.when(down_waits & down_next)
        def _():
            signal(relay.at[1], below)

        signal(relay.at[3], side)
        pl.semaphore_wait(relay.at[3], 1)
        signal(relay.at[2], across)

    half = part.shape[0] // 2
    chunk = half // mates
    mine = pl.ds(parity * half, half)
    his = pl.ds((1 - parity) * half, half)

    def piece(idx):
        return pl.ds(pl.multiple_of(parity * half + idx * chunk, 8), chunk)

    own = piece(h)

    def g_pair():
        return push(part.at[his], pair_in, g_send.at[0], g_recv.at[0], partner)

    def g_ring(k):
        return push(part.at[piece(mate(k))], ring_in.at[k], g_send.at[0],
                    g_recv.at[1], at(mate(k), c))

    def g_cross():
        return push(gram.at[own], gram.at[own], g_send.at[0], g_recv.at[2], (side[0], other))

    held = piece(h + c * (1 - 2 * lax.rem(h, 2)))

    def g_gather(k):
        return push(gram.at[held], gram.at[held], g_send.at[1], g_recv.at[3], at(mate(k), c))

    def g_half(rows):
        return push(gram.at[rows], gram.at[rows], g_send.at[1], g_recv.at[4], partner)

    def amount(ref, send_sem, recv_sem):
        return push(ref, ref, send_sem, recv_sem, partner)

    owners = range(mates)
    split = mates // 2
    rows_chunk = size // mates

    def rows_at(offset, count):
        return pl.ds(pl.multiple_of(offset, 8), count)

    y_mine = rows_at(parity * size, size)
    y_his = rows_at((1 - parity) * size, size)

    def y_piece(idx):
        return rows_at(parity * size + idx * rows_chunk, rows_chunk)

    def y_pair(q):
        if q < 2:
            src, dst = xy.at[q, y_his], xy_pair.at[q]
        else:
            rows = rows_at((1 - parity) * size + (q - 2) * part_rows, part_rows)
            src, dst = xy.at[:, rows], xy_pair.at[:, pl.ds((q - 2) * part_rows, part_rows)]
        return push(src, dst, y_send.at[0], y_recv.at[q % 2], partner)

    def y_merge(q):
        if q < 2:
            xy[q, y_mine] = xy[q, y_mine] + xy_pair[q]
        else:
            rows = rows_at(parity * size + (q - 2) * part_rows, part_rows)
            span = pl.ds((q - 2) * part_rows, part_rows)
            xy[:, rows] = xy[:, rows] + xy_pair[:, span]

    near, far, share, lend, final = range(2, 7)

    def y_near(j):
        return push(xy.at[c, y_piece(j)], xy_ring.at[0, h], y_send.at[1],
                    y_recv.at[near], at(j, c))

    def y_far(j):
        return push(xy.at[other, y_piece(j)], xy_ring.at[1, h], y_send.at[0],
                    y_recv.at[far], at(j, other))

    def y_share(j):
        view = xy_all.at[c, y_piece(h)]
        return push(view, view, y_send.at[1], y_recv.at[share], at(j, c))

    def y_lend(j):
        view = xy_all.at[c, y_piece(h)]
        return push(view, view, y_send.at[1], y_recv.at[lend], at(j, other))

    def y_half(which, plane, rows):
        view = xy_all.at[plane, rows]
        return push(view, view, y_send.at[2], y_recv.at[final + which], partner)

    lends = (c == 0) | (parity == 0)
    borrows = (c == 1) | (parity == 0)

    def unless_self(j, step):
        @pl.when(h != j)
        def _():
            step()

    def scatter(q):
        y_pair(q).wait_recv()
        y_merge(q)
        if q in (1, 3):
            for j in owners:
                y_far(j).start()
        if q != 1:
            for j in owners:
                if q == 0 or (j >= split) == (q == 3):
                    unless_self(j, y_near(j).start)

    def meet(q):
        if q < 2:
            xy[q] = across_rows(xs[:, early], ys[q * size:(q + 1) * size, early])
        else:
            groups = (top, bottom)[q - 2]
            value = across_rows(
                jnp.concatenate([xs[rows, late] for rows in groups], axis=0), ys[:, late])
            for g, rows in enumerate(groups):
                block = value[g * part_rows:(g + 1) * part_rows]
                xy[0, rows] = block[:, :size]
                xy[1, rows] = block[:, size:]
        y_pair(q).start()

    @pl.when(c == 0)
    def _():
        for q in range(2):
            load_copy(q, xs).wait()
            span = early if q == 0 else late
            strip = across_rows(xs[:size, span], xs[:, span])
            rest = across_rows(xs[size:, span], xs[size:, span])
            if q == 0:
                part[:size] = strip[:, :size]
                part[size:2 * size] = strip[:, size:]
                part[2 * size:] = rest
            else:
                part[:size] = part[:size] + strip[:, :size]
                part[size:2 * size] = part[size:2 * size] + strip[:, size:]
                part[2 * size:] = part[2 * size:] + rest
        g_pair().start()

    everyone()

    @pl.when(c == 0)
    def _():
        g_pair().wait_recv()
        part[mine] = part[mine] + pair_in[...]
        for k in range(1, mates):
            g_ring(k).start()
        amount(ring_in.at[pl.ds(1, mates - 1)], g_send.at[0], g_recv.at[1]).wait_recv()
        total = part[own]
        for k in range(1, mates):
            total = total + ring_in[k]
        gram[own] = total
        g_cross().start()

    @pl.when(c == 1)
    def _():
        for q in range(2):
            load_copy(q, ys).wait()
        x_group_wait(0)
        meet(2)
        pl.semaphore_wait(relay.at[2], 1)
        scatter(2)
        amount(gram.at[held], g_send.at[0], g_recv.at[2]).wait_recv()

    for k in range(1, mates):
        g_gather(k).start()

    @pl.when(c == 0)
    def _():
        y_copy(0).wait_recv()
        meet(0)

    @pl.when(c == 1)
    def _():
        x_group_wait(1)
        meet(3)
        scatter(3)

    amount(gram.at[pl.ds(0, (mates - 1) * chunk)], g_send.at[1], g_recv.at[3]).wait_recv()
    g_half(mine).start()

    @pl.when(c == 0)
    def _():
        scatter(0)

    g_half(his).wait_recv()

    eye = (lax.broadcasted_iota(jnp.int32, (size, size), 0)
           == lax.broadcasted_iota(jnp.int32, (size, size), 1)).astype(jnp.float32)
    first[:, :size] = gram[:size]
    first[:, size:2 * size] = gram[size:2 * size]
    first[:, 2 * size:] = eye

    def on_plane(plane, step):
        @pl.when(c == plane)
        def _():
            step()

    def meet_last():
        x_copy(5).start()
        y_copy(1).wait_recv()
        meet(1)

    def scatter_last():
        pl.semaphore_wait(relay.at[2], 1)
        scatter(1)
        for q in range(6, 9):
            x_copy(q).start()

    def gather():
        amount(xy_ring.at[0, pl.ds(0, mates - 1)], y_send.at[1], y_recv.at[near]).wait_recv()
        amount(xy_ring.at[1], y_send.at[0], y_recv.at[far]).wait_recv()
        total = xy[c, y_piece(h)]
        for k in range(1, mates):
            total = total + xy_ring[0, mate(k)]
        for j in range(mates):
            total = total + xy_ring[1, j]
        xy_all[c, y_piece(h)] = total
        for j in range(mates):
            unless_self(j, y_share(j).start)

        @pl.when(lends)
        def _():
            for j in range(mates):
                y_lend(j).start()

    eliminate(first, {
        0: lambda: on_plane(0, meet_last),
        2: lambda: on_plane(0, scatter_last),
        7: lambda: on_plane(1, gather),
    })

    upper = first[:, size:2 * size]
    cross = contract(upper, first[:, size:], ((0,), (0,)))
    second[:, :size] = gram[2 * size:] - cross[:, :size]
    second[:, size:2 * size] = -cross[:, size:]
    second[:, 2 * size:] = eye
    eliminate(second, {
        3: lambda: on_plane(0, gather),
    })

    inverse[:size, :size] = first[:, 2 * size:]
    inverse[:size, size:] = jnp.zeros((size, size), jnp.float32)
    inverse[size:] = second[:, size:]
    own_rows = pl.ds(pl.multiple_of(c * size, size), size)
    factors[:size] = inverse[own_rows]
    factors[size:] = contract(inverse[...], inverse[...], ((0,), (0,)))

    def products(lo, count):
        span = pl.ds(lo * eighth, count * eighth)
        q_ref[:, span] = product(factors[:size], xs[:, span]) * scaling
        z_ref[:, span] = product(factors[size:], xs[:, span])

    keep = (lax.broadcasted_iota(jnp.int32, (size, size), 0)
            <= lax.broadcasted_iota(jnp.int32, (size, size), 1))

    def trail(lo, count):
        span = cols(lo, count)
        tail_ref[:, span] = ys[own_rows, span] - contract(
            xy_all[c], z_ref[:, span], ((0,), (0,)))

    @pl.when(c == 0)
    def _():
        tri_ref[:, :size] = jnp.where(keep, first[:, :size], 0.0) / scaling
        tri_ref[:, size:2 * size] = first[:, size:2 * size] / scaling
        y_copy(2).wait_recv()

    @pl.when(c == 1)
    def _():
        tri_ref[:, :size] = jnp.zeros((size, size), jnp.float32)
        tri_ref[:, size:2 * size] = jnp.where(keep, second[:, :size], 0.0) / scaling

    inv_ref[...] = factors[:size]
    def rows_of(count):
        return xy_all.at[0, pl.ds(0, count * rows_chunk)]

    def take_own():
        amount(rows_of(mates - 1), y_send.at[1], y_recv.at[share]).wait_recv()
        y_half(0, c, y_mine).start()

    def take_other():
        amount(rows_of(mates), y_send.at[1], y_recv.at[lend]).wait_recv()
        y_half(1, other, y_mine).start()

    def sent():
        amount(gram.at[pl.ds(0, (mates - 1) * chunk + half)], g_send.at[1],
               g_recv.at[0]).wait_send()
        amount(part, y_send.at[0], y_recv.at[0]).wait_send()
        amount(xy_pair.at[0], y_send.at[2], y_recv.at[0]).wait_send()

        @pl.when(lends)
        def _():
            amount(part.at[pl.ds(0, (3 * mates - 2) * rows_chunk)], y_send.at[1],
                   y_recv.at[0]).wait_send()

        @pl.when(jnp.logical_not(lends))
        def _():
            amount(part.at[pl.ds(0, (2 * mates - 2) * rows_chunk)], y_send.at[1],
                   y_recv.at[0]).wait_send()

        sum_ref[c] = xy_all[c]

    products(4, 4)

    @pl.when(c == 0)
    def _():
        products(0, 4)
        amount(part, g_send.at[0], g_recv.at[0]).wait_send()
        take_own()
        y_half(0, c, y_his).wait_recv()
        sum_ref[1, size:] = jnp.zeros((size, size), jnp.float32)
        trail(0, 8)
        bulk_sent()
        sent()

        @pl.when(borrows)
        def _():
            take_other()
            sum_ref[1, :size] = xy_all[1, :size]
            y_half(1, other, y_mine).wait_send()

        @pl.when(jnp.logical_not(borrows))
        def _():
            y_half(1, other, y_his).wait_recv()
            sum_ref[1, :size] = xy_all[1, :size]

    @pl.when(c == 1)
    def _():
        take_own()
        x_group_wait(2)
        products(0, 3)
        x_group_wait(3)
        products(3, 1)
        take_other()
        bulk_sent()
        y_half(0, c, y_his).wait_recv()
        trail(0, 8)
        sent()
        y_half(1, other, y_his).wait_recv()
        sum_ref[0] = xy_all[0]
        y_half(1, other, y_mine).wait_send()


def finish_kernel(scaling, q_in, tail_in, tri_in, inv_ref, sum_ref,
                  ortho_ref, tri_ref, trail_ref, right, sems):
    size = tri_in.shape[0]

    def out(k, src, dst):
        return pltpu.make_async_copy(src, dst, sems.at[k])

    copies = [
        out(0, q_in, ortho_ref),
        out(1, tail_in, trail_ref),
        out(2, tri_in, tri_ref.at[:, :2 * size]),
        out(3, right, tri_ref.at[:, 2 * size:]),
    ]
    for copy in copies[:3]:
        copy.start()
    right[:, :size] = product(inv_ref[...], sum_ref[0]) / scaling
    right[:, size:] = product(inv_ref[...], sum_ref[1]) / scaling
    copies[3].start()
    for copy in copies:
        copy.wait()


def fused(columns):
    row_count = lax.axis_size("rows")
    width = columns.shape[1]
    scaling = math.sqrt(width * row_count)
    size = PANEL
    mates = row_count // 2
    f32 = jnp.float32
    vmem = pl.BlockSpec(memory_space=pltpu.VMEM)
    ortho = jax.ShapeDtypeStruct((size, width), f32)
    triangle = jax.ShapeDtypeStruct((size, 4 * size), f32)
    trailing = ortho
    middle = pl.pallas_call(
        functools.partial(kernel, row_count, scaling),
        out_shape=(
            ortho,
            trailing,
            jax.ShapeDtypeStruct((size, 2 * size), f32),
            jax.ShapeDtypeStruct((size, 2 * size), f32),
            jax.ShapeDtypeStruct((2, 2 * size, size), f32),
        ),
        in_specs=[pl.BlockSpec(memory_space=pltpu.HBM)],
        out_specs=(vmem,) * 5,
        scratch_shapes=[
            pltpu.VMEM((2 * size, width), f32),
            pltpu.VMEM((2 * size, width), f32),
            pltpu.VMEM((3 * size, size), f32),
            pltpu.VMEM((3 * size, size), f32),
            pltpu.VMEM((3 * size // 2, size), f32),
            pltpu.VMEM((mates, 3 * size // row_count, size), f32),
            pltpu.VMEM((size, 3 * size), f32),
            pltpu.VMEM((size, 3 * size), f32),
            pltpu.VMEM((2 * size, 2 * size), f32),
            pltpu.VMEM((3 * size, 2 * size), f32),
            pltpu.VMEM((2 * size, width), f32),
            pltpu.VMEM((2, 2 * size, size), f32),
            pltpu.VMEM((2, size, size), f32),
            pltpu.VMEM((2, mates, size // mates, size), f32),
            pltpu.VMEM((2, 2 * size, size), f32),
            pltpu.SemaphoreType.DMA((2,)),
            pltpu.SemaphoreType.DMA((1,)),
            pltpu.SemaphoreType.DMA((4,)),
            pltpu.SemaphoreType.DMA((2,)),
            pltpu.SemaphoreType.DMA((5,)),
            pltpu.SemaphoreType.DMA((3,)),
            pltpu.SemaphoreType.DMA((8,)),
            pltpu.SemaphoreType.REGULAR((4,)),
        ],
        compiler_params=pltpu.CompilerParams(
            collective_id=0, has_side_effects=True, vmem_limit_bytes=VMEM_BYTES),
    )(pltpu.with_memory_space_constraint(columns, pltpu.HBM))
    return pl.pallas_call(
        functools.partial(finish_kernel, scaling),
        out_shape=(ortho, triangle, trailing),
        in_specs=[vmem] * 5,
        out_specs=(pl.BlockSpec(memory_space=pltpu.HBM),) * 3,
        scratch_shapes=[
            pltpu.VMEM((size, 2 * size), f32),
            pltpu.SemaphoreType.DMA((4,)),
        ],
        compiler_params=pltpu.CompilerParams(vmem_limit_bytes=VMEM_BYTES),
    )(*middle)


def inverse_lower(lower):
    identity = jnp.eye(lower.shape[0], dtype=lower.dtype)
    return lax.linalg.triangular_solve(lower, identity, left_side=True, lower=True)


def summed(partial_term):
    return lax.psum(partial_term, "rows")


def general(columns):
    col_count = lax.axis_size("cols")
    col_index = lax.axis_index("cols")
    scaling = math.sqrt(columns.shape[1] * lax.axis_size("rows"))
    local_rows = lax.all_gather(columns, "cols", axis=0, tiled=True)
    panel_count = 2 * PANEL
    leading = local_rows[:panel_count]
    gram_strip = summed(product(leading, local_rows.T))
    lower_both = jnp.linalg.cholesky(gram_strip[:, :panel_count])
    inverse_both = inverse_lower(lower_both)
    orthonormal = product(inverse_both, leading)
    coupling = product(inverse_both, gram_strip[:, panel_count:])
    trailing = local_rows[panel_count:] - product(coupling.T, orthonormal)
    triangle = jnp.concatenate([lower_both.T, coupling], axis=1)
    orthonormal = orthonormal * scaling
    triangle = triangle / scaling

    def own(array):
        count = array.shape[0] // col_count
        return lax.dynamic_slice_in_dim(array, col_index * count, count, 0)

    return (own(orthonormal), own(triangle), own(trailing))


def shards(columns):
    rows = lax.axis_size("rows")
    paired = lax.axis_size("cols") == 2 and columns.shape[0] == 2 * PANEL and columns.shape[1] % (8 * PANEL) == 0
    if paired and rows % 8 == 0 and (2 * PANEL) % (8 * rows) == 0 and (3 * PANEL) % (8 * rows) == 0:
        return fused(columns)
    return general(columns)


def solution(mesh):
    placed = (P("cols", "rows"),)
    return jax.shard_map(
        shards,
        mesh=mesh,
        in_specs=placed,
        out_specs=(P("cols", "rows"), P("cols", None), P("cols", "rows")),
        check_vma=False,
    )
```

```python
import functools
import math

import jax
import jax.numpy as jnp
from jax import lax
from jax.experimental import pallas as pl
from jax.experimental.pallas import tpu as pltpu
from jax.sharding import PartitionSpec as P

PANEL = 128
STRIP = 16
VMEM_BYTES = 20 * 2**20
MESH = pl.DeviceIdType.MESH

precise = lax.Precision.HIGHEST


def product(left, right):
    return jnp.dot(left, right, precision=precise, preferred_element_type=jnp.float32)


def contract(left, right, dims):
    return lax.dot_general(
        left, right, (dims, ((), ())), precision=precise, preferred_element_type=jnp.float32
    )


def across_rows(left, right):
    return contract(left, right, ((1,), (1,)))


def pieces(value):
    first = value.astype(jnp.bfloat16)
    rest = value - first.astype(jnp.float32)
    second = rest.astype(jnp.bfloat16)
    third = (rest - second.astype(jnp.float32)).astype(jnp.bfloat16)
    return first, second, third


def strip_update(left, right, after):
    a, b, c = pieces(left)
    d, e, f = pieces(right)
    lhs = jnp.concatenate([a, a, b, a, c, b], axis=0)
    rhs = jnp.concatenate([d, e, d, f, d, e], axis=0)
    return jnp.dot(lhs.T[after:], rhs, preferred_element_type=jnp.float32)


def spread(value, i):
    return jnp.broadcast_to(value[i:i + 1], value.shape)


def eliminate(ref, hooks):
    size = ref.shape[0]
    lanes = size
    parts = ref.shape[1] // lanes
    tall = STRIP // 2
    below = lax.broadcasted_iota(jnp.int32, (tall, lanes), 0)

    def column(value, j):
        return jnp.broadcast_to(value[:, j:j + 1], (tall, lanes))

    def diagonal(cols):
        value = cols[0]
        for j in range(1, tall):
            value = jnp.where(below == j, cols[j], value)
        return value

    for s in range(size // STRIP):
        at = s * STRIP
        spans = [slice(q * lanes, (q + 1) * lanes) for q in range(parts)]
        upper = [ref[at:at + tall, span] for span in spans]
        lower = [ref[at + tall:at + STRIP, span] for span in spans]
        tops = [column(upper[0], at + j) for j in range(tall)]
        lows = [column(lower[0], at + j) for j in range(STRIP)]
        scale_top = lax.rsqrt(diagonal(tops))
        scale_low = lax.rsqrt(diagonal(lows[tall:]))
        upper = [value * scale_top for value in upper]
        lower = [value * scale_low for value in lower]
        for j in range(STRIP):
            own_scale = spread(scale_top if j < tall else scale_low, j % tall)
            lows[j] = lows[j] * scale_low * own_scale
            if j < tall:
                tops[j] = tops[j] * scale_top * own_scale
        for i in range(0, STRIP, 2):
            high = i < tall
            r = i % tall
            cur = tops if high else lows
            rows = upper if high else lower
            corner = spread(cur[i], r)
            edge = spread(cur[i], r + 1)
            minor = corner * spread(cur[i + 1], r + 1) - edge * edge
            inv = lax.rsqrt(corner)
            inv_next = lax.rsqrt(minor) * (corner * inv)
            slope = edge * inv
            col = cur[i] * inv
            col_next = (cur[i + 1] - col * slope) * inv_next
            coef = jnp.where(below > r, col, 0.0)
            coef_next = jnp.where(below > r + 1, col_next, 0.0)
            if high:
                tail = lows[i] * inv
                tail_next = (lows[i + 1] - tail * slope) * inv_next
            for j in range(i + 2, STRIP):
                same = high == (j < tall)
                one = spread(col if same else tail, j % tall)
                two = spread(col_next if same else tail_next, j % tall)
                if same:
                    cur[j] = (cur[j] - coef * one) - coef_next * two
                if high:
                    lows[j] = (lows[j] - tail * one) - tail_next * two
            for q in range(parts):
                row = spread(rows[q], r) * inv
                rest = rows[q] - coef * row
                row_next = spread(rest, r + 1) * inv_next
                rest = jnp.where(below == r + 1, row_next, rest - coef_next * row_next)
                rows[q] = jnp.where(below == r, row, rest)
                if high:
                    lower[q] = (lower[q] - tail * row) - tail_next * row_next
        rows = [jnp.concatenate([upper[q], lower[q]], axis=0) for q in range(parts)]
        for q in range(parts):
            ref[at:at + STRIP, spans[q]] = rows[q]
        after = at + STRIP
        if after < size:
            update = strip_update(rows[0], jnp.concatenate(rows, axis=1), after)
            ref[after:, :] = ref[after:, :] - update
        if s in hooks:
            hooks[s]()


def kernel(row_count, scaling, x_ref, q_ref, tail_ref, tri_ref, inv_ref, sum_ref,
           xs, ys, part, gram, pair_in, ring_in, first, second, inverse, factors, z_ref,
           xy, xy_pair, xy_ring, xy_all, load, x_send, x_recv, g_send, g_recv,
           y_send, y_recv, relay):
    r = lax.axis_index("rows")
    c = lax.axis_index("cols")
    other = 1 - c
    parity = lax.rem(r, 2)
    h = r // 2
    mates = row_count // 2
    line = mates // 2
    place = h // 2
    partner = (r + 1 - 2 * parity, c)
    across = (r, other)
    side = ((h + 1 - 2 * lax.rem(h, 2)) * 2 + parity, c)
    above = (r + 4, c)
    below = (r - 4, c)
    has_above = place < line - 1
    has_below = place > 0
    size = PANEL
    width = xs.shape[1]
    half_width = width // 2
    eighth = width // 8

    def mate(k):
        return lax.rem(h + k, mates)

    def at(idx, plane):
        return (idx * 2 + parity, plane)

    def push(src, dst, send_sem, recv_sem, target):
        return pltpu.make_async_remote_copy(
            src_ref=src, dst_ref=dst, send_sem=send_sem, recv_sem=recv_sem,
            device_id=target, device_id_type=MESH)

    def signal(sem, target):
        pl.semaphore_signal(sem, inc=1, device_id=target, device_id_type=MESH)

    barrier = pltpu.get_barrier_semaphore()
    for target in (across, partner, side):
        signal(barrier, target)

    @pl.when(has_above)
    def _():
        signal(barrier, above)

    @pl.when(has_below)
    def _():
        signal(barrier, below)

    early = pl.ds(0, half_width)
    late = pl.ds(half_width, half_width)

    def load_copy(q, dst):
        span = early if q == 0 else late
        return pltpu.make_async_copy(x_ref.at[:, span], dst.at[:, span], load.at[q])

    @pl.when(c == 0)
    def _():
        for q in range(2):
            load_copy(q, xs).start()

    @pl.when(c == 1)
    def _():
        for q in range(2):
            load_copy(q, ys).start()

    pl.semaphore_wait(barrier, 3 + has_above.astype(jnp.int32) + has_below.astype(jnp.int32))

    part_rows = size // 2
    top = [pl.ds(q * size, part_rows) for q in range(2)]
    bottom = [pl.ds(q * size + part_rows, part_rows) for q in range(2)]
    every = pl.ds(0, 2 * size)

    def cols(lo, count):
        return pl.ds(lo * eighth, count * eighth)

    x_views = (
        [(rows, late) for rows in top]
        + [(rows, late) for rows in bottom]
        + [(every, cols(0, 1)), (pl.ds(0, size), cols(1, 1)), (pl.ds(size, size), cols(1, 1)),
           (every, cols(2, 1)), (every, cols(3, 1))]
    )
    y_views = [(pl.ds(0, size), early), (pl.ds(size, size), early), (pl.ds(0, size), late)]

    x_group = (0, 0, 1, 1, 2, 2, 2, 2, 3)

    def x_copy(q):
        return push(x_ref.at[x_views[q]], xs.at[x_views[q]], x_send.at[0],
                    x_recv.at[x_group[q]], across)

    def y_copy(q):
        return push(x_ref.at[y_views[q]], ys.at[y_views[q]], x_send.at[0], x_recv.at[q], across)

    def bulk(ref, send_sem, recv_sem):
        return push(ref, ref, send_sem, recv_sem, across)

    x_sizes = ((size, late), (size, late), (2 * size, cols(0, 3)),
               (2 * size, cols(3, 1)))

    def x_group_wait(g):
        rows, span = x_sizes[g]
        bulk(xs.at[pl.ds(0, rows), span], x_send.at[0], x_recv.at[g]).wait_recv()

    def bulk_sent():
        @pl.when(c == 0)
        def _():
            bulk(xs, x_send.at[0], x_recv.at[0]).wait_send()

        @pl.when(c == 1)
        def _():
            bulk(ys.at[pl.ds(0, 3 * size // 2)], x_send.at[0], x_recv.at[0]).wait_send()

    @pl.when(c == 0)
    def _():
        for q in range(5):
            x_copy(q).start()

    @pl.when(c == 1)
    def _():
        for q in range(3):
            y_copy(q).start()

    up_next = has_below & has_above
    up_waits = place > 1
    down_next = has_above & has_below
    down_waits = place < line - 2

    @pl.when(up_next & jnp.logical_not(up_waits))
    def _():
        signal(relay.at[0], above)

    @pl.when(down_next & jnp.logical_not(down_waits))
    def _():
        signal(relay.at[1], below)

    def everyone():
        @pl.when(up_waits)
        def _():
            pl.semaphore_wait(relay.at[0], 1)

        @pl.when(up_waits & up_next)
        def _():
            signal(relay.at[0], above)

        @pl.when(down_waits)
        def _():
            pl.semaphore_wait(relay.at[1], 1)

        @pl.when(down_waits & down_next)
        def _():
            signal(relay.at[1], below)

        signal(relay.at[3], side)
        pl.semaphore_wait(relay.at[3], 1)
        signal(relay.at[2], across)

    half = part.shape[0] // 2
    chunk = half // mates
    mine = pl.ds(parity * half, half)
    his = pl.ds((1 - parity) * half, half)

    def piece(idx):
        return pl.ds(pl.multiple_of(parity * half + idx * chunk, 8), chunk)

    own = piece(h)

    def g_pair():
        return push(part.at[his], pair_in, g_send.at[0], g_recv.at[0], partner)

    def g_ring(k):
        return push(part.at[piece(mate(k))], ring_in.at[k], g_send.at[0],
                    g_recv.at[1], at(mate(k), c))

    def g_cross():
        return push(gram.at[own], gram.at[own], g_send.at[0], g_recv.at[2], (side[0], other))

    held = piece(h + c * (1 - 2 * lax.rem(h, 2)))

    def g_gather(k):
        return push(gram.at[held], gram.at[held], g_send.at[1], g_recv.at[3], at(mate(k), c))

    def g_half(rows):
        return push(gram.at[rows], gram.at[rows], g_send.at[1], g_recv.at[4], partner)

    def amount(ref, send_sem, recv_sem):
        return push(ref, ref, send_sem, recv_sem, partner)

    owners = range(mates)
    split = mates // 2
    rows_chunk = size // mates

    def rows_at(offset, count):
        return pl.ds(pl.multiple_of(offset, 8), count)

    y_mine = rows_at(parity * size, size)
    y_his = rows_at((1 - parity) * size, size)

    def y_piece(idx):
        return rows_at(parity * size + idx * rows_chunk, rows_chunk)

    def y_pair(q):
        if q < 2:
            src, dst = xy.at[q, y_his], xy_pair.at[q]
        else:
            rows = rows_at((1 - parity) * size + (q - 2) * part_rows, part_rows)
            src, dst = xy.at[:, rows], xy_pair.at[:, pl.ds((q - 2) * part_rows, part_rows)]
        return push(src, dst, y_send.at[0], y_recv.at[q % 2], partner)

    def y_merge(q):
        if q < 2:
            xy[q, y_mine] = xy[q, y_mine] + xy_pair[q]
        else:
            rows = rows_at(parity * size + (q - 2) * part_rows, part_rows)
            span = pl.ds((q - 2) * part_rows, part_rows)
            xy[:, rows] = xy[:, rows] + xy_pair[:, span]

    near, far, share, lend, final = range(2, 7)

    def y_near(j):
        return push(xy.at[c, y_piece(j)], xy_ring.at[0, h], y_send.at[1],
                    y_recv.at[near], at(j, c))

    def y_far(j):
        return push(xy.at[other, y_piece(j)], xy_ring.at[1, h], y_send.at[0],
                    y_recv.at[far], at(j, other))

    def y_share(j):
        view = xy_all.at[c, y_piece(h)]
        return push(view, view, y_send.at[1], y_recv.at[share], at(j, c))

    def y_lend(j, side_core=0):
        view = xy_all.at[c, y_piece(h)]
        row = j * 2 + (1 - parity if side_core else parity)
        return push(view, view, y_send.at[1], y_recv.at[lend], (row, other))

    def y_half(which, plane, rows):
        view = xy_all.at[plane, rows]
        return push(view, view, y_send.at[2], y_recv.at[final + which], partner)

    def unless_self(j, step):
        @pl.when(h != j)
        def _():
            step()

    def scatter(q):
        y_pair(q).wait_recv()
        y_merge(q)
        if q in (1, 3):
            for j in owners:
                y_far(j).start()
        if q != 1:
            for j in owners:
                if q == 0 or (j >= split) == (q == 3):
                    unless_self(j, y_near(j).start)

    def meet(q):
        if q < 2:
            xy[q] = across_rows(xs[:, early], ys[q * size:(q + 1) * size, early])
        else:
            groups = (top, bottom)[q - 2]
            value = across_rows(
                jnp.concatenate([xs[rows, late] for rows in groups], axis=0), ys[:, late])
            for g, rows in enumerate(groups):
                block = value[g * part_rows:(g + 1) * part_rows]
                xy[0, rows] = block[:, :size]
                xy[1, rows] = block[:, size:]
        y_pair(q).start()

    @pl.when(c == 0)
    def _():
        for q in range(2):
            load_copy(q, xs).wait()
            span = early if q == 0 else late
            strip = across_rows(xs[:size, span], xs[:, span])
            rest = across_rows(xs[size:, span], xs[size:, span])
            if q == 0:
                part[:size] = strip[:, :size]
                part[size:2 * size] = strip[:, size:]
                part[2 * size:] = rest
            else:
                part[:size] = part[:size] + strip[:, :size]
                part[size:2 * size] = part[size:2 * size] + strip[:, size:]
                part[2 * size:] = part[2 * size:] + rest
        g_pair().start()

    everyone()

    @pl.when(c == 0)
    def _():
        g_pair().wait_recv()
        part[mine] = part[mine] + pair_in[...]
        for k in range(1, mates):
            g_ring(k).start()
        amount(ring_in.at[pl.ds(1, mates - 1)], g_send.at[0], g_recv.at[1]).wait_recv()
        total = part[own]
        for k in range(1, mates):
            total = total + ring_in[k]
        gram[own] = total
        g_cross().start()

    @pl.when(c == 1)
    def _():
        for q in range(2):
            load_copy(q, ys).wait()
        x_group_wait(0)
        meet(2)
        pl.semaphore_wait(relay.at[2], 1)
        scatter(2)
        amount(gram.at[held], g_send.at[0], g_recv.at[2]).wait_recv()

    for k in range(1, mates):
        g_gather(k).start()

    @pl.when(c == 0)
    def _():
        y_copy(0).wait_recv()
        meet(0)

    @pl.when(c == 1)
    def _():
        x_group_wait(1)
        meet(3)
        scatter(3)

    amount(gram.at[pl.ds(0, (mates - 1) * chunk)], g_send.at[1], g_recv.at[3]).wait_recv()
    g_half(mine).start()

    @pl.when(c == 0)
    def _():
        scatter(0)

    g_half(his).wait_recv()

    eye = (lax.broadcasted_iota(jnp.int32, (size, size), 0)
           == lax.broadcasted_iota(jnp.int32, (size, size), 1)).astype(jnp.float32)
    first[:, :size] = gram[:size]
    first[:, size:2 * size] = gram[size:2 * size]
    first[:, 2 * size:] = eye

    def on_plane(plane, step):
        @pl.when(c == plane)
        def _():
            step()

    def meet_last():
        for q in range(5, 7):
            x_copy(q).start()
        y_copy(1).wait_recv()
        meet(1)

    def scatter_last():
        pl.semaphore_wait(relay.at[2], 1)
        scatter(1)
        for q in range(7, 9):
            x_copy(q).start()

    def gather():
        amount(xy_ring.at[0, pl.ds(0, mates - 1)], y_send.at[1], y_recv.at[near]).wait_recv()
        amount(xy_ring.at[1], y_send.at[0], y_recv.at[far]).wait_recv()
        total = xy[c, y_piece(h)]
        for k in range(1, mates):
            total = total + xy_ring[0, mate(k)]
        for j in range(mates):
            total = total + xy_ring[1, j]
        xy_all[c, y_piece(h)] = total
        for j in range(mates):
            unless_self(j, y_share(j).start)

        @pl.when(c == 0)
        def _():
            for j in range(mates):
                y_lend(j).start()

        @pl.when((c == 1) & (parity == 0))
        def _():
            for j in range(mates):
                for core in range(2):
                    y_lend(j, core).start()

    eliminate(first, {
        0: lambda: on_plane(0, meet_last),
        2: lambda: on_plane(0, scatter_last),
        7: lambda: on_plane(1, gather),
    })

    upper = first[:, size:2 * size]
    cross = contract(upper, first[:, size:], ((0,), (0,)))
    second[:, :size] = gram[2 * size:] - cross[:, :size]
    second[:, size:2 * size] = -cross[:, size:]
    second[:, 2 * size:] = eye
    eliminate(second, {
        3: lambda: on_plane(0, gather),
    })

    inverse[:size, :size] = first[:, 2 * size:]
    inverse[:size, size:] = jnp.zeros((size, size), jnp.float32)
    inverse[size:] = second[:, size:]
    own_rows = pl.ds(pl.multiple_of(c * size, size), size)
    factors[:size] = inverse[own_rows]
    factors[size:] = contract(inverse[...], inverse[...], ((0,), (0,)))

    def products(lo, count):
        span = pl.ds(lo * eighth, count * eighth)
        q_ref[:, span] = product(factors[:size], xs[:, span]) * scaling
        z_ref[:, span] = product(factors[size:], xs[:, span])

    keep = (lax.broadcasted_iota(jnp.int32, (size, size), 0)
            <= lax.broadcasted_iota(jnp.int32, (size, size), 1))

    def trail(lo, count):
        span = cols(lo, count)
        tail_ref[:, span] = ys[own_rows, span] - contract(
            xy_all[c], z_ref[:, span], ((0,), (0,)))

    @pl.when(c == 0)
    def _():
        tri_ref[:, :size] = jnp.where(keep, first[:, :size], 0.0) / scaling
        tri_ref[:, size:2 * size] = first[:, size:2 * size] / scaling
        y_copy(2).wait_recv()

    @pl.when(c == 1)
    def _():
        tri_ref[:, :size] = jnp.zeros((size, size), jnp.float32)
        tri_ref[:, size:2 * size] = jnp.where(keep, second[:, :size], 0.0) / scaling

    inv_ref[...] = factors[:size]
    def rows_of(count):
        return xy_all.at[0, pl.ds(0, count * rows_chunk)]

    def take_own():
        amount(rows_of(mates - 1), y_send.at[1], y_recv.at[share]).wait_recv()
        y_half(0, c, y_mine).start()

    def take_other():
        amount(rows_of(mates), y_send.at[1], y_recv.at[lend]).wait_recv()

    def sent(pieces_sent):
        rows = pieces_sent * rows_chunk // 2
        amount(xy.at[:, pl.ds(0, rows)], y_send.at[1], y_recv.at[0]).wait_send()

    def all_sent():
        amount(gram.at[pl.ds(0, (mates - 1) * chunk + half)], g_send.at[1],
               g_recv.at[0]).wait_send()
        amount(part, y_send.at[0], y_recv.at[0]).wait_send()
        bulk_sent()
        sum_ref[c] = xy_all[c]

    products(4, 4)

    @pl.when(c == 0)
    def _():
        products(0, 4)
        amount(part, g_send.at[0], g_recv.at[0]).wait_send()
        take_own()
        y_half(0, c, y_his).wait_recv()
        sum_ref[1, size:] = jnp.zeros((size, size), jnp.float32)
        trail(0, 8)
        all_sent()
        amount(xy_pair.at[0], y_send.at[2], y_recv.at[0]).wait_send()
        sent(3 * mates - 2)
        take_other()
        sum_ref[1, :size] = xy_all[1, :size]

    @pl.when(c == 1)
    def _():
        take_own()
        for g in range(2, 4):
            x_group_wait(g)
        products(0, 4)
        take_other()
        y_half(1, other, y_mine).start()
        y_half(0, c, y_his).wait_recv()
        trail(0, 8)
        all_sent()

        @pl.when(parity == 0)
        def _():
            sent(4 * mates - 2)

        @pl.when(parity == 1)
        def _():
            sent(2 * mates - 2)

        y_half(1, other, y_his).wait_recv()
        sum_ref[0] = xy_all[0]
        amount(xy_pair, y_send.at[2], y_recv.at[0]).wait_send()


def finish_kernel(scaling, q_in, tail_in, tri_in, inv_ref, sum_ref,
                  ortho_ref, tri_ref, trail_ref, right, sems):
    size = tri_in.shape[0]

    def out(k, src, dst):
        return pltpu.make_async_copy(src, dst, sems.at[k])

    copies = [
        out(0, q_in, ortho_ref),
        out(1, tail_in, trail_ref),
        out(2, tri_in, tri_ref.at[:, :2 * size]),
        out(3, right, tri_ref.at[:, 2 * size:]),
    ]
    for copy in copies[:3]:
        copy.start()
    right[:, :size] = product(inv_ref[...], sum_ref[0]) / scaling
    right[:, size:] = product(inv_ref[...], sum_ref[1]) / scaling
    copies[3].start()
    for copy in copies:
        copy.wait()


def fused(columns):
    row_count = lax.axis_size("rows")
    width = columns.shape[1]
    scaling = math.sqrt(width * row_count)
    size = PANEL
    mates = row_count // 2
    f32 = jnp.float32
    vmem = pl.BlockSpec(memory_space=pltpu.VMEM)
    ortho = jax.ShapeDtypeStruct((size, width), f32)
    triangle = jax.ShapeDtypeStruct((size, 4 * size), f32)
    trailing = ortho
    middle = pl.pallas_call(
        functools.partial(kernel, row_count, scaling),
        out_shape=(
            ortho,
            trailing,
            jax.ShapeDtypeStruct((size, 2 * size), f32),
            jax.ShapeDtypeStruct((size, 2 * size), f32),
            jax.ShapeDtypeStruct((2, 2 * size, size), f32),
        ),
        in_specs=[pl.BlockSpec(memory_space=pltpu.HBM)],
        out_specs=(vmem,) * 5,
        scratch_shapes=[
            pltpu.VMEM((2 * size, width), f32),
            pltpu.VMEM((2 * size, width), f32),
            pltpu.VMEM((3 * size, size), f32),
            pltpu.VMEM((3 * size, size), f32),
            pltpu.VMEM((3 * size // 2, size), f32),
            pltpu.VMEM((mates, 3 * size // row_count, size), f32),
            pltpu.VMEM((size, 3 * size), f32),
            pltpu.VMEM((size, 3 * size), f32),
            pltpu.VMEM((2 * size, 2 * size), f32),
            pltpu.VMEM((3 * size, 2 * size), f32),
            pltpu.VMEM((2 * size, width), f32),
            pltpu.VMEM((2, 2 * size, size), f32),
            pltpu.VMEM((2, size, size), f32),
            pltpu.VMEM((2, mates, size // mates, size), f32),
            pltpu.VMEM((2, 2 * size, size), f32),
            pltpu.SemaphoreType.DMA((2,)),
            pltpu.SemaphoreType.DMA((1,)),
            pltpu.SemaphoreType.DMA((4,)),
            pltpu.SemaphoreType.DMA((2,)),
            pltpu.SemaphoreType.DMA((5,)),
            pltpu.SemaphoreType.DMA((3,)),
            pltpu.SemaphoreType.DMA((8,)),
            pltpu.SemaphoreType.REGULAR((4,)),
        ],
        compiler_params=pltpu.CompilerParams(
            collective_id=0, has_side_effects=True, vmem_limit_bytes=VMEM_BYTES),
    )(pltpu.with_memory_space_constraint(columns, pltpu.HBM))
    return pl.pallas_call(
        functools.partial(finish_kernel, scaling),
        out_shape=(ortho, triangle, trailing),
        in_specs=[vmem] * 5,
        out_specs=(pl.BlockSpec(memory_space=pltpu.HBM),) * 3,
        scratch_shapes=[
            pltpu.VMEM((size, 2 * size), f32),
            pltpu.SemaphoreType.DMA((4,)),
        ],
        compiler_params=pltpu.CompilerParams(vmem_limit_bytes=VMEM_BYTES),
    )(*middle)


def inverse_lower(lower):
    identity = jnp.eye(lower.shape[0], dtype=lower.dtype)
    return lax.linalg.triangular_solve(lower, identity, left_side=True, lower=True)


def summed(partial_term):
    return lax.psum(partial_term, "rows")


def general(columns):
    col_count = lax.axis_size("cols")
    col_index = lax.axis_index("cols")
    scaling = math.sqrt(columns.shape[1] * lax.axis_size("rows"))
    local_rows = lax.all_gather(columns, "cols", axis=0, tiled=True)
    panel_count = 2 * PANEL
    leading = local_rows[:panel_count]
    gram_strip = summed(product(leading, local_rows.T))
    lower_both = jnp.linalg.cholesky(gram_strip[:, :panel_count])
    inverse_both = inverse_lower(lower_both)
    orthonormal = product(inverse_both, leading)
    coupling = product(inverse_both, gram_strip[:, panel_count:])
    trailing = local_rows[panel_count:] - product(coupling.T, orthonormal)
    triangle = jnp.concatenate([lower_both.T, coupling], axis=1)
    orthonormal = orthonormal * scaling
    triangle = triangle / scaling

    def own(array):
        count = array.shape[0] // col_count
        return lax.dynamic_slice_in_dim(array, col_index * count, count, 0)

    return (own(orthonormal), own(triangle), own(trailing))


def shards(columns):
    rows = lax.axis_size("rows")
    paired = lax.axis_size("cols") == 2 and columns.shape[0] == 2 * PANEL and columns.shape[1] % (8 * PANEL) == 0
    if paired and rows % 8 == 0 and (2 * PANEL) % (8 * rows) == 0 and (3 * PANEL) % (8 * rows) == 0:
        return fused(columns)
    return general(columns)


def solution(mesh):
    placed = (P("cols", "rows"),)
    return jax.shard_map(
        shards,
        mesh=mesh,
        in_specs=placed,
        out_specs=(P("cols", "rows"), P("cols", None), P("cols", "rows")),
        check_vma=False,
    )
```

```python
import functools
import math

import jax
import jax.numpy as jnp
from jax import lax
from jax.experimental import pallas as pl
from jax.experimental.pallas import tpu as pltpu
from jax.sharding import PartitionSpec as P

PANEL = 128
STRIP = 16
VMEM_BYTES = 20 * 2**20
MESH = pl.DeviceIdType.MESH

precise = lax.Precision.HIGHEST


def product(left, right):
    return jnp.dot(left, right, precision=precise, preferred_element_type=jnp.float32)


def contract(left, right, dims):
    return lax.dot_general(
        left, right, (dims, ((), ())), precision=precise, preferred_element_type=jnp.float32
    )


def across_rows(left, right):
    return contract(left, right, ((1,), (1,)))


def pieces(value):
    first = value.astype(jnp.bfloat16)
    rest = value - first.astype(jnp.float32)
    second = rest.astype(jnp.bfloat16)
    third = (rest - second.astype(jnp.float32)).astype(jnp.bfloat16)
    return first, second, third


def strip_update(left, right, after):
    a, b, c = pieces(left)
    d, e, f = pieces(right)
    lhs = jnp.concatenate([a, a, b, a, c, b], axis=0)
    rhs = jnp.concatenate([d, e, d, f, d, e], axis=0)
    return jnp.dot(lhs.T[after:], rhs, preferred_element_type=jnp.float32)


def spread(value, i):
    return jnp.broadcast_to(value[i:i + 1], value.shape)


def eliminate(ref, hooks):
    size = ref.shape[0]
    lanes = size
    parts = ref.shape[1] // lanes
    tall = STRIP // 2
    below = lax.broadcasted_iota(jnp.int32, (tall, lanes), 0)

    def column(value, j):
        return jnp.broadcast_to(value[:, j:j + 1], (tall, lanes))

    def diagonal(cols):
        value = cols[0]
        for j in range(1, tall):
            value = jnp.where(below == j, cols[j], value)
        return value

    for s in range(size // STRIP):
        at = s * STRIP
        spans = [slice(q * lanes, (q + 1) * lanes) for q in range(parts)]
        upper = [ref[at:at + tall, span] for span in spans]
        lower = [ref[at + tall:at + STRIP, span] for span in spans]
        tops = [column(upper[0], at + j) for j in range(tall)]
        lows = [column(lower[0], at + j) for j in range(STRIP)]
        scale_top = lax.rsqrt(diagonal(tops))
        scale_low = lax.rsqrt(diagonal(lows[tall:]))
        upper = [value * scale_top for value in upper]
        lower = [value * scale_low for value in lower]
        for j in range(STRIP):
            own_scale = spread(scale_top if j < tall else scale_low, j % tall)
            lows[j] = lows[j] * scale_low * own_scale
            if j < tall:
                tops[j] = tops[j] * scale_top * own_scale
        for i in range(0, STRIP, 2):
            high = i < tall
            r = i % tall
            cur = tops if high else lows
            rows = upper if high else lower
            corner = spread(cur[i], r)
            edge = spread(cur[i], r + 1)
            minor = corner * spread(cur[i + 1], r + 1) - edge * edge
            inv = lax.rsqrt(corner)
            inv_next = lax.rsqrt(minor) * (corner * inv)
            slope = edge * inv
            col = cur[i] * inv
            col_next = (cur[i + 1] - col * slope) * inv_next
            coef = jnp.where(below > r, col, 0.0)
            coef_next = jnp.where(below > r + 1, col_next, 0.0)
            if high:
                tail = lows[i] * inv
                tail_next = (lows[i + 1] - tail * slope) * inv_next
            for j in range(i + 2, STRIP):
                same = high == (j < tall)
                one = spread(col if same else tail, j % tall)
                two = spread(col_next if same else tail_next, j % tall)
                if same:
                    cur[j] = (cur[j] - coef * one) - coef_next * two
                if high:
                    lows[j] = (lows[j] - tail * one) - tail_next * two
            for q in range(parts):
                row = spread(rows[q], r) * inv
                rest = rows[q] - coef * row
                row_next = spread(rest, r + 1) * inv_next
                rest = jnp.where(below == r + 1, row_next, rest - coef_next * row_next)
                rows[q] = jnp.where(below == r, row, rest)
                if high:
                    lower[q] = (lower[q] - tail * row) - tail_next * row_next
        rows = [jnp.concatenate([upper[q], lower[q]], axis=0) for q in range(parts)]
        for q in range(parts):
            ref[at:at + STRIP, spans[q]] = rows[q]
        after = at + STRIP
        if after < size:
            update = strip_update(rows[0], jnp.concatenate(rows, axis=1), after)
            ref[after:, :] = ref[after:, :] - update
        if s in hooks:
            hooks[s]()


def kernel(row_count, scaling, x_ref, q_ref, tail_ref, tri_ref, inv_ref, sum_ref,
           xs, ys, part, gram, pair_in, ring_in, first, second, inverse, factors, z_ref,
           xy, xy_pair, xy_ring, xy_all, load, x_send, x_recv, g_send, g_recv,
           y_send, y_recv, relay):
    r = lax.axis_index("rows")
    c = lax.axis_index("cols")
    other = 1 - c
    parity = lax.rem(r, 2)
    h = r // 2
    mates = row_count // 2
    line = mates // 2
    place = h // 2
    partner = (r + 1 - 2 * parity, c)
    across = (r, other)
    side = ((h + 1 - 2 * lax.rem(h, 2)) * 2 + parity, c)
    above = (r + 4, c)
    below = (r - 4, c)
    has_above = place < line - 1
    has_below = place > 0
    size = PANEL
    width = xs.shape[1]
    half_width = width // 2
    eighth = width // 8

    def mate(k):
        return lax.rem(h + k, mates)

    def at(idx, plane):
        return (idx * 2 + parity, plane)

    def push(src, dst, send_sem, recv_sem, target):
        return pltpu.make_async_remote_copy(
            src_ref=src, dst_ref=dst, send_sem=send_sem, recv_sem=recv_sem,
            device_id=target, device_id_type=MESH)

    def signal(sem, target):
        pl.semaphore_signal(sem, inc=1, device_id=target, device_id_type=MESH)

    barrier = pltpu.get_barrier_semaphore()
    for target in (across, partner, side):
        signal(barrier, target)

    @pl.when(has_above)
    def _():
        signal(barrier, above)

    @pl.when(has_below)
    def _():
        signal(barrier, below)

    early = pl.ds(0, half_width)
    late = pl.ds(half_width, half_width)

    def load_copy(q, dst):
        span = early if q == 0 else late
        return pltpu.make_async_copy(x_ref.at[:, span], dst.at[:, span], load.at[q])

    @pl.when(c == 0)
    def _():
        for q in range(2):
            load_copy(q, xs).start()

    @pl.when(c == 1)
    def _():
        for q in range(2):
            load_copy(q, ys).start()

    pl.semaphore_wait(barrier, 3 + has_above.astype(jnp.int32) + has_below.astype(jnp.int32))

    part_rows = size // 2
    top = [pl.ds(q * size, part_rows) for q in range(2)]
    bottom = [pl.ds(q * size + part_rows, part_rows) for q in range(2)]
    every = pl.ds(0, 2 * size)

    def cols(lo, count):
        return pl.ds(lo * eighth, count * eighth)

    x_views = (
        [(rows, late) for rows in top]
        + [(rows, late) for rows in bottom]
        + [(every, cols(0, 1)), (pl.ds(0, size), cols(1, 1)), (pl.ds(size, size), cols(1, 1)),
           (every, cols(2, 1)), (every, cols(3, 1))]
    )
    y_views = [(pl.ds(0, size), early), (pl.ds(size, size), early), (pl.ds(0, size), late)]

    x_group = (0, 0, 1, 1, 2, 2, 2, 2, 3)

    def x_copy(q):
        return push(x_ref.at[x_views[q]], xs.at[x_views[q]], x_send.at[0],
                    x_recv.at[x_group[q]], across)

    def y_copy(q):
        return push(x_ref.at[y_views[q]], ys.at[y_views[q]], x_send.at[0], x_recv.at[q], across)

    def bulk(ref, send_sem, recv_sem):
        return push(ref, ref, send_sem, recv_sem, across)

    x_sizes = ((size, late), (size, late), (2 * size, cols(0, 3)),
               (2 * size, cols(3, 1)))

    def x_group_wait(g):
        rows, span = x_sizes[g]
        bulk(xs.at[pl.ds(0, rows), span], x_send.at[0], x_recv.at[g]).wait_recv()

    def bulk_sent():
        @pl.when(c == 0)
        def _():
            bulk(xs, x_send.at[0], x_recv.at[0]).wait_send()

        @pl.when(c == 1)
        def _():
            bulk(ys.at[pl.ds(0, 3 * size // 2)], x_send.at[0], x_recv.at[0]).wait_send()

    @pl.when(c == 0)
    def _():
        for q in range(5):
            x_copy(q).start()

    @pl.when(c == 1)
    def _():
        for q in range(3):
            y_copy(q).start()

    up_next = has_below & has_above
    up_waits = place > 1
    down_next = has_above & has_below
    down_waits = place < line - 2

    @pl.when(up_next & jnp.logical_not(up_waits))
    def _():
        signal(relay.at[0], above)

    @pl.when(down_next & jnp.logical_not(down_waits))
    def _():
        signal(relay.at[1], below)

    def everyone():
        @pl.when(up_waits)
        def _():
            pl.semaphore_wait(relay.at[0], 1)

        @pl.when(up_waits & up_next)
        def _():
            signal(relay.at[0], above)

        @pl.when(down_waits)
        def _():
            pl.semaphore_wait(relay.at[1], 1)

        @pl.when(down_waits & down_next)
        def _():
            signal(relay.at[1], below)

        signal(relay.at[3], side)
        pl.semaphore_wait(relay.at[3], 1)
        signal(relay.at[2], across)

    half = part.shape[0] // 2
    chunk = half // mates
    mine = pl.ds(parity * half, half)
    his = pl.ds((1 - parity) * half, half)

    def piece(idx):
        return pl.ds(pl.multiple_of(parity * half + idx * chunk, 8), chunk)

    own = piece(h)

    def g_pair():
        return push(part.at[his], pair_in, g_send.at[0], g_recv.at[0], partner)

    def g_ring(k):
        return push(part.at[piece(mate(k))], ring_in.at[k], g_send.at[0],
                    g_recv.at[1], at(mate(k), c))

    def g_cross():
        return push(gram.at[own], gram.at[own], g_send.at[0], g_recv.at[2], (side[0], other))

    held = piece(h + c * (1 - 2 * lax.rem(h, 2)))

    def g_gather(k):
        return push(gram.at[held], gram.at[held], g_send.at[1], g_recv.at[3], at(mate(k), c))

    def g_half(rows):
        return push(gram.at[rows], gram.at[rows], g_send.at[1], g_recv.at[4], partner)

    def amount(ref, send_sem, recv_sem):
        return push(ref, ref, send_sem, recv_sem, partner)

    owners = range(mates)
    split = mates // 2
    rows_chunk = size // mates

    def rows_at(offset, count):
        return pl.ds(pl.multiple_of(offset, 8), count)

    y_mine = rows_at(parity * size, size)
    y_his = rows_at((1 - parity) * size, size)

    def y_piece(idx):
        return rows_at(parity * size + idx * rows_chunk, rows_chunk)

    def y_pair(q):
        if q < 2:
            src, dst = xy.at[q, y_his], xy_pair.at[q]
        else:
            rows = rows_at((1 - parity) * size + (q - 2) * part_rows, part_rows)
            src, dst = xy.at[:, rows], xy_pair.at[:, pl.ds((q - 2) * part_rows, part_rows)]
        return push(src, dst, y_send.at[0], y_recv.at[q % 2], partner)

    def y_merge(q):
        if q < 2:
            xy[q, y_mine] = xy[q, y_mine] + xy_pair[q]
        else:
            rows = rows_at(parity * size + (q - 2) * part_rows, part_rows)
            span = pl.ds((q - 2) * part_rows, part_rows)
            xy[:, rows] = xy[:, rows] + xy_pair[:, span]

    near, far, share, lend, final = range(2, 7)

    def y_near(j):
        return push(xy.at[c, y_piece(j)], xy_ring.at[0, h], y_send.at[1],
                    y_recv.at[near], at(j, c))

    def y_far(j):
        return push(xy.at[other, y_piece(j)], xy_ring.at[1, h], y_send.at[0],
                    y_recv.at[far], at(j, other))

    def y_share(j):
        view = xy_all.at[c, y_piece(h)]
        return push(view, view, y_send.at[1], y_recv.at[share], at(j, c))

    def y_lend(j, side_core=0):
        view = xy_all.at[c, y_piece(h)]
        row = j * 2 + (1 - parity if side_core else parity)
        return push(view, view, y_send.at[1], y_recv.at[lend], (row, other))

    def y_half(which, plane, rows):
        view = xy_all.at[plane, rows]
        return push(view, view, y_send.at[2], y_recv.at[final + which], partner)

    def unless_self(j, step):
        @pl.when(h != j)
        def _():
            step()

    def scatter(q):
        y_pair(q).wait_recv()
        y_merge(q)
        if q in (1, 3):
            for j in owners:
                y_far(j).start()
        if q != 1:
            for j in owners:
                if q == 0 or (j >= split) == (q == 3):
                    unless_self(j, y_near(j).start)

    def meet(q):
        if q < 2:
            xy[q] = across_rows(xs[:, early], ys[q * size:(q + 1) * size, early])
        else:
            groups = (top, bottom)[q - 2]
            value = across_rows(
                jnp.concatenate([xs[rows, late] for rows in groups], axis=0), ys[:, late])
            for g, rows in enumerate(groups):
                block = value[g * part_rows:(g + 1) * part_rows]
                xy[0, rows] = block[:, :size]
                xy[1, rows] = block[:, size:]
        y_pair(q).start()

    @pl.when(c == 0)
    def _():
        for q in range(2):
            load_copy(q, xs).wait()
            span = early if q == 0 else late
            strip = across_rows(xs[:size, span], xs[:, span])
            rest = across_rows(xs[size:, span], xs[size:, span])
            if q == 0:
                part[:size] = strip[:, :size]
                part[size:2 * size] = strip[:, size:]
                part[2 * size:] = rest
            else:
                part[:size] = part[:size] + strip[:, :size]
                part[size:2 * size] = part[size:2 * size] + strip[:, size:]
                part[2 * size:] = part[2 * size:] + rest
        g_pair().start()

    everyone()

    @pl.when(c == 0)
    def _():
        g_pair().wait_recv()
        part[mine] = part[mine] + pair_in[...]
        for k in range(1, mates):
            g_ring(k).start()
        amount(ring_in.at[pl.ds(1, mates - 1)], g_send.at[0], g_recv.at[1]).wait_recv()
        total = part[own]
        for k in range(1, mates):
            total = total + ring_in[k]
        gram[own] = total
        g_cross().start()

    @pl.when(c == 1)
    def _():
        for q in range(2):
            load_copy(q, ys).wait()
        x_group_wait(0)
        meet(2)
        pl.semaphore_wait(relay.at[2], 1)
        scatter(2)
        amount(gram.at[held], g_send.at[0], g_recv.at[2]).wait_recv()

    for k in range(1, mates):
        g_gather(k).start()

    @pl.when(c == 0)
    def _():
        y_copy(0).wait_recv()
        meet(0)

    @pl.when(c == 1)
    def _():
        x_group_wait(1)
        meet(3)
        scatter(3)

    amount(gram.at[pl.ds(0, (mates - 1) * chunk)], g_send.at[1], g_recv.at[3]).wait_recv()
    g_half(mine).start()

    @pl.when(c == 0)
    def _():
        scatter(0)
        for q in range(5, 7):
            x_copy(q).start()

    g_half(his).wait_recv()

    eye = (lax.broadcasted_iota(jnp.int32, (size, size), 0)
           == lax.broadcasted_iota(jnp.int32, (size, size), 1)).astype(jnp.float32)
    first[:, :size] = gram[:size]
    first[:, size:2 * size] = gram[size:2 * size]
    first[:, 2 * size:] = eye

    def on_plane(plane, step):
        @pl.when(c == plane)
        def _():
            step()

    def meet_last():
        y_copy(1).wait_recv()
        meet(1)

    def scatter_last():
        pl.semaphore_wait(relay.at[2], 1)
        scatter(1)
        for q in range(7, 9):
            x_copy(q).start()

    def gather():
        amount(xy_ring.at[0, pl.ds(0, mates - 1)], y_send.at[1], y_recv.at[near]).wait_recv()
        amount(xy_ring.at[1], y_send.at[0], y_recv.at[far]).wait_recv()
        total = xy[c, y_piece(h)]
        for k in range(1, mates):
            total = total + xy_ring[0, mate(k)]
        for j in range(mates):
            total = total + xy_ring[1, j]
        xy_all[c, y_piece(h)] = total
        for j in range(mates):
            unless_self(j, y_share(j).start)

        @pl.when(c == 0)
        def _():
            for j in range(mates):
                y_lend(j).start()

        @pl.when((c == 1) & (parity == 0))
        def _():
            for j in range(mates):
                for core in range(2):
                    y_lend(j, core).start()

    eliminate(first, {
        0: lambda: on_plane(0, meet_last),
        2: lambda: on_plane(0, scatter_last),
        7: lambda: on_plane(1, gather),
    })

    upper = first[:, size:2 * size]
    cross = contract(upper, first[:, size:], ((0,), (0,)))
    second[:, :size] = gram[2 * size:] - cross[:, :size]
    second[:, size:2 * size] = -cross[:, size:]
    second[:, 2 * size:] = eye
    eliminate(second, {
        3: lambda: on_plane(0, gather),
    })

    inverse[:size, :size] = first[:, 2 * size:]
    inverse[:size, size:] = jnp.zeros((size, size), jnp.float32)
    inverse[size:] = second[:, size:]
    own_rows = pl.ds(pl.multiple_of(c * size, size), size)
    factors[:size] = inverse[own_rows]
    factors[size:] = contract(inverse[...], inverse[...], ((0,), (0,)))

    def products(lo, count):
        span = pl.ds(lo * eighth, count * eighth)
        q_ref[:, span] = product(factors[:size], xs[:, span]) * scaling
        z_ref[:, span] = product(factors[size:], xs[:, span])

    keep = (lax.broadcasted_iota(jnp.int32, (size, size), 0)
            <= lax.broadcasted_iota(jnp.int32, (size, size), 1))

    def trail(lo, count):
        span = cols(lo, count)
        tail_ref[:, span] = ys[own_rows, span] - contract(
            xy_all[c], z_ref[:, span], ((0,), (0,)))

    @pl.when(c == 0)
    def _():
        tri_ref[:, :size] = jnp.where(keep, first[:, :size], 0.0) / scaling
        tri_ref[:, size:2 * size] = first[:, size:2 * size] / scaling
        y_copy(2).wait_recv()

    @pl.when(c == 1)
    def _():
        tri_ref[:, :size] = jnp.zeros((size, size), jnp.float32)
        tri_ref[:, size:2 * size] = jnp.where(keep, second[:, :size], 0.0) / scaling

    inv_ref[...] = factors[:size]
    def rows_of(count):
        return xy_all.at[0, pl.ds(0, count * rows_chunk)]

    def take_own():
        amount(rows_of(mates - 1), y_send.at[1], y_recv.at[share]).wait_recv()
        y_half(0, c, y_mine).start()

    def take_other():
        amount(rows_of(mates), y_send.at[1], y_recv.at[lend]).wait_recv()

    def sent(pieces_sent):
        rows = pieces_sent * rows_chunk // 2
        amount(xy.at[:, pl.ds(0, rows)], y_send.at[1], y_recv.at[0]).wait_send()

    def all_sent():
        amount(gram.at[pl.ds(0, (mates - 1) * chunk + half)], g_send.at[1],
               g_recv.at[0]).wait_send()
        amount(part, y_send.at[0], y_recv.at[0]).wait_send()
        bulk_sent()
        sum_ref[c] = xy_all[c]

    products(4, 4)

    @pl.when(c == 0)
    def _():
        products(0, 4)
        amount(part, g_send.at[0], g_recv.at[0]).wait_send()
        take_own()
        y_half(0, c, y_his).wait_recv()
        sum_ref[1, size:] = jnp.zeros((size, size), jnp.float32)
        trail(0, 8)
        all_sent()
        amount(xy_pair.at[0], y_send.at[2], y_recv.at[0]).wait_send()
        sent(3 * mates - 2)
        take_other()
        sum_ref[1, :size] = xy_all[1, :size]

    @pl.when(c == 1)
    def _():
        take_own()
        for g in range(2, 4):
            x_group_wait(g)
        products(0, 4)
        take_other()
        y_half(1, other, y_mine).start()
        y_half(0, c, y_his).wait_recv()
        trail(0, 8)
        all_sent()

        @pl.when(parity == 0)
        def _():
            sent(4 * mates - 2)

        @pl.when(parity == 1)
        def _():
            sent(2 * mates - 2)

        y_half(1, other, y_his).wait_recv()
        sum_ref[0] = xy_all[0]
        amount(xy_pair, y_send.at[2], y_recv.at[0]).wait_send()


def finish_kernel(scaling, q_in, tail_in, tri_in, inv_ref, sum_ref,
                  ortho_ref, tri_ref, trail_ref, right, sems):
    size = tri_in.shape[0]

    def out(k, src, dst):
        return pltpu.make_async_copy(src, dst, sems.at[k])

    copies = [
        out(0, q_in, ortho_ref),
        out(1, tail_in, trail_ref),
        out(2, tri_in, tri_ref.at[:, :2 * size]),
        out(3, right, tri_ref.at[:, 2 * size:]),
    ]
    for copy in copies[:3]:
        copy.start()
    right[:, :size] = product(inv_ref[...], sum_ref[0]) / scaling
    right[:, size:] = product(inv_ref[...], sum_ref[1]) / scaling
    copies[3].start()
    for copy in copies:
        copy.wait()


def fused(columns):
    row_count = lax.axis_size("rows")
    width = columns.shape[1]
    scaling = math.sqrt(width * row_count)
    size = PANEL
    mates = row_count // 2
    f32 = jnp.float32
    vmem = pl.BlockSpec(memory_space=pltpu.VMEM)
    ortho = jax.ShapeDtypeStruct((size, width), f32)
    triangle = jax.ShapeDtypeStruct((size, 4 * size), f32)
    trailing = ortho
    middle = pl.pallas_call(
        functools.partial(kernel, row_count, scaling),
        out_shape=(
            ortho,
            trailing,
            jax.ShapeDtypeStruct((size, 2 * size), f32),
            jax.ShapeDtypeStruct((size, 2 * size), f32),
            jax.ShapeDtypeStruct((2, 2 * size, size), f32),
        ),
        in_specs=[pl.BlockSpec(memory_space=pltpu.HBM)],
        out_specs=(vmem,) * 5,
        scratch_shapes=[
            pltpu.VMEM((2 * size, width), f32),
            pltpu.VMEM((2 * size, width), f32),
            pltpu.VMEM((3 * size, size), f32),
            pltpu.VMEM((3 * size, size), f32),
            pltpu.VMEM((3 * size // 2, size), f32),
            pltpu.VMEM((mates, 3 * size // row_count, size), f32),
            pltpu.VMEM((size, 3 * size), f32),
            pltpu.VMEM((size, 3 * size), f32),
            pltpu.VMEM((2 * size, 2 * size), f32),
            pltpu.VMEM((3 * size, 2 * size), f32),
            pltpu.VMEM((2 * size, width), f32),
            pltpu.VMEM((2, 2 * size, size), f32),
            pltpu.VMEM((2, size, size), f32),
            pltpu.VMEM((2, mates, size // mates, size), f32),
            pltpu.VMEM((2, 2 * size, size), f32),
            pltpu.SemaphoreType.DMA((2,)),
            pltpu.SemaphoreType.DMA((1,)),
            pltpu.SemaphoreType.DMA((4,)),
            pltpu.SemaphoreType.DMA((2,)),
            pltpu.SemaphoreType.DMA((5,)),
            pltpu.SemaphoreType.DMA((3,)),
            pltpu.SemaphoreType.DMA((8,)),
            pltpu.SemaphoreType.REGULAR((4,)),
        ],
        compiler_params=pltpu.CompilerParams(
            collective_id=0, has_side_effects=True, vmem_limit_bytes=VMEM_BYTES),
    )(pltpu.with_memory_space_constraint(columns, pltpu.HBM))
    return pl.pallas_call(
        functools.partial(finish_kernel, scaling),
        out_shape=(ortho, triangle, trailing),
        in_specs=[vmem] * 5,
        out_specs=(pl.BlockSpec(memory_space=pltpu.HBM),) * 3,
        scratch_shapes=[
            pltpu.VMEM((size, 2 * size), f32),
            pltpu.SemaphoreType.DMA((4,)),
        ],
        compiler_params=pltpu.CompilerParams(vmem_limit_bytes=VMEM_BYTES),
    )(*middle)


def inverse_lower(lower):
    identity = jnp.eye(lower.shape[0], dtype=lower.dtype)
    return lax.linalg.triangular_solve(lower, identity, left_side=True, lower=True)


def summed(partial_term):
    return lax.psum(partial_term, "rows")


def general(columns):
    col_count = lax.axis_size("cols")
    col_index = lax.axis_index("cols")
    scaling = math.sqrt(columns.shape[1] * lax.axis_size("rows"))
    local_rows = lax.all_gather(columns, "cols", axis=0, tiled=True)
    panel_count = 2 * PANEL
    leading = local_rows[:panel_count]
    gram_strip = summed(product(leading, local_rows.T))
    lower_both = jnp.linalg.cholesky(gram_strip[:, :panel_count])
    inverse_both = inverse_lower(lower_both)
    orthonormal = product(inverse_both, leading)
    coupling = product(inverse_both, gram_strip[:, panel_count:])
    trailing = local_rows[panel_count:] - product(coupling.T, orthonormal)
    triangle = jnp.concatenate([lower_both.T, coupling], axis=1)
    orthonormal = orthonormal * scaling
    triangle = triangle / scaling

    def own(array):
        count = array.shape[0] // col_count
        return lax.dynamic_slice_in_dim(array, col_index * count, count, 0)

    return (own(orthonormal), own(triangle), own(trailing))


def shards(columns):
    rows = lax.axis_size("rows")
    paired = lax.axis_size("cols") == 2 and columns.shape[0] == 2 * PANEL and columns.shape[1] % (8 * PANEL) == 0
    if paired and rows % 8 == 0 and (2 * PANEL) % (8 * rows) == 0 and (3 * PANEL) % (8 * rows) == 0:
        return fused(columns)
    return general(columns)


def solution(mesh):
    placed = (P("cols", "rows"),)
    return jax.shard_map(
        shards,
        mesh=mesh,
        in_specs=placed,
        out_specs=(P("cols", "rows"), P("cols", None), P("cols", "rows")),
        check_vma=False,
    )
```

```python
import functools
import math

import jax
import jax.numpy as jnp
from jax import lax
from jax.experimental import pallas as pl
from jax.experimental.pallas import tpu as pltpu
from jax.sharding import PartitionSpec as P

PANEL = 128
STRIP = 16
VMEM_BYTES = 20 * 2**20
MESH = pl.DeviceIdType.MESH

precise = lax.Precision.HIGHEST


def product(left, right):
    return jnp.dot(left, right, precision=precise, preferred_element_type=jnp.float32)


def contract(left, right, dims):
    return lax.dot_general(
        left, right, (dims, ((), ())), precision=precise, preferred_element_type=jnp.float32
    )


def across_rows(left, right):
    return contract(left, right, ((1,), (1,)))


def pieces(value):
    first = value.astype(jnp.bfloat16)
    rest = value - first.astype(jnp.float32)
    second = rest.astype(jnp.bfloat16)
    third = (rest - second.astype(jnp.float32)).astype(jnp.bfloat16)
    return first, second, third


def strip_update(left, right, after):
    a, b, c = pieces(left)
    d, e, f = pieces(right)
    lhs = jnp.concatenate([a, a, b, a, c, b], axis=0)
    rhs = jnp.concatenate([d, e, d, f, d, e], axis=0)
    return jnp.dot(lhs.T[after:], rhs, preferred_element_type=jnp.float32)


def spread(value, i):
    return jnp.broadcast_to(value[i:i + 1], value.shape)


def eliminate(ref, hooks):
    size = ref.shape[0]
    lanes = size
    parts = ref.shape[1] // lanes
    tall = STRIP // 2
    below = lax.broadcasted_iota(jnp.int32, (tall, lanes), 0)

    def column(value, j):
        return jnp.broadcast_to(value[:, j:j + 1], (tall, lanes))

    def diagonal(cols):
        value = cols[0]
        for j in range(1, tall):
            value = jnp.where(below == j, cols[j], value)
        return value

    for s in range(size // STRIP):
        at = s * STRIP
        spans = [slice(q * lanes, (q + 1) * lanes) for q in range(parts)]
        upper = [ref[at:at + tall, span] for span in spans]
        lower = [ref[at + tall:at + STRIP, span] for span in spans]
        tops = [column(upper[0], at + j) for j in range(tall)]
        lows = [column(lower[0], at + j) for j in range(STRIP)]
        scale_top = lax.rsqrt(diagonal(tops))
        scale_low = lax.rsqrt(diagonal(lows[tall:]))
        upper = [value * scale_top for value in upper]
        lower = [value * scale_low for value in lower]
        for j in range(STRIP):
            own_scale = spread(scale_top if j < tall else scale_low, j % tall)
            lows[j] = lows[j] * scale_low * own_scale
            if j < tall:
                tops[j] = tops[j] * scale_top * own_scale
        for i in range(0, STRIP, 2):
            high = i < tall
            r = i % tall
            cur = tops if high else lows
            rows = upper if high else lower
            corner = spread(cur[i], r)
            edge = spread(cur[i], r + 1)
            minor = corner * spread(cur[i + 1], r + 1) - edge * edge
            inv = lax.rsqrt(corner)
            inv_next = lax.rsqrt(minor) * (corner * inv)
            slope = edge * inv
            col = cur[i] * inv
            col_next = (cur[i + 1] - col * slope) * inv_next
            coef = jnp.where(below > r, col, 0.0)
            coef_next = jnp.where(below > r + 1, col_next, 0.0)
            if high:
                tail = lows[i] * inv
                tail_next = (lows[i + 1] - tail * slope) * inv_next
            for j in range(i + 2, STRIP):
                same = high == (j < tall)
                one = spread(col if same else tail, j % tall)
                two = spread(col_next if same else tail_next, j % tall)
                if same:
                    cur[j] = (cur[j] - coef * one) - coef_next * two
                if high:
                    lows[j] = (lows[j] - tail * one) - tail_next * two
            for q in range(parts):
                row = spread(rows[q], r) * inv
                rest = rows[q] - coef * row
                row_next = spread(rest, r + 1) * inv_next
                rest = jnp.where(below == r + 1, row_next, rest - coef_next * row_next)
                rows[q] = jnp.where(below == r, row, rest)
                if high:
                    lower[q] = (lower[q] - tail * row) - tail_next * row_next
        rows = [jnp.concatenate([upper[q], lower[q]], axis=0) for q in range(parts)]
        for q in range(parts):
            ref[at:at + STRIP, spans[q]] = rows[q]
        after = at + STRIP
        if after < size:
            update = strip_update(rows[0], jnp.concatenate(rows, axis=1), after)
            ref[after:, :] = ref[after:, :] - update
        if s in hooks:
            hooks[s]()


def kernel(row_count, scaling, x_ref, q_ref, tail_ref, tri_ref, inv_ref, sum_ref,
           xs, ys, part, gram, pair_in, ring_in, first, second, inverse, factors, z_ref,
           xy, xy_pair, xy_ring, xy_all, load, x_send, x_recv, g_send, g_recv,
           y_send, y_recv, relay):
    r = lax.axis_index("rows")
    c = lax.axis_index("cols")
    other = 1 - c
    parity = lax.rem(r, 2)
    h = r // 2
    mates = row_count // 2
    line = mates // 2
    place = h // 2
    partner = (r + 1 - 2 * parity, c)
    across = (r, other)
    side = ((h + 1 - 2 * lax.rem(h, 2)) * 2 + parity, c)
    above = (r + 4, c)
    below = (r - 4, c)
    has_above = place < line - 1
    has_below = place > 0
    size = PANEL
    width = xs.shape[1]
    half_width = width // 2
    eighth = width // 8

    def mate(k):
        return lax.rem(h + k, mates)

    def at(idx, plane):
        return (idx * 2 + parity, plane)

    def push(src, dst, send_sem, recv_sem, target):
        return pltpu.make_async_remote_copy(
            src_ref=src, dst_ref=dst, send_sem=send_sem, recv_sem=recv_sem,
            device_id=target, device_id_type=MESH)

    def signal(sem, target):
        pl.semaphore_signal(sem, inc=1, device_id=target, device_id_type=MESH)

    barrier = pltpu.get_barrier_semaphore()
    for target in (across, partner, side):
        signal(barrier, target)

    @pl.when(has_above)
    def _():
        signal(barrier, above)

    @pl.when(has_below)
    def _():
        signal(barrier, below)

    early = pl.ds(0, half_width)
    late = pl.ds(half_width, half_width)

    def load_copy(q, dst):
        span = early if q == 0 else late
        return pltpu.make_async_copy(x_ref.at[:, span], dst.at[:, span], load.at[q])

    @pl.when(c == 0)
    def _():
        for q in range(2):
            load_copy(q, xs).start()

    @pl.when(c == 1)
    def _():
        for q in range(2):
            load_copy(q, ys).start()

    pl.semaphore_wait(barrier, 3 + has_above.astype(jnp.int32) + has_below.astype(jnp.int32))

    part_rows = size // 2
    top = [pl.ds(q * size, part_rows) for q in range(2)]
    bottom = [pl.ds(q * size + part_rows, part_rows) for q in range(2)]
    every = pl.ds(0, 2 * size)

    def cols(lo, count):
        return pl.ds(lo * eighth, count * eighth)

    x_views = (
        [(rows, late) for rows in top]
        + [(rows, late) for rows in bottom]
        + [(every, cols(0, 1)), (pl.ds(0, size), cols(1, 1)), (pl.ds(size, size), cols(1, 1)),
           (every, cols(2, 1)), (every, cols(3, 1))]
    )
    y_views = [(pl.ds(0, size), early), (pl.ds(size, size), early), (pl.ds(0, size), late)]

    x_group = (0, 0, 1, 1, 2, 2, 2, 2, 3)

    def x_copy(q):
        return push(x_ref.at[x_views[q]], xs.at[x_views[q]], x_send.at[0],
                    x_recv.at[x_group[q]], across)

    def y_copy(q):
        return push(x_ref.at[y_views[q]], ys.at[y_views[q]], x_send.at[0], x_recv.at[q], across)

    def bulk(ref, send_sem, recv_sem):
        return push(ref, ref, send_sem, recv_sem, across)

    x_sizes = ((size, late), (size, late), (2 * size, cols(0, 3)),
               (2 * size, cols(3, 1)))

    def x_group_wait(g):
        rows, span = x_sizes[g]
        bulk(xs.at[pl.ds(0, rows), span], x_send.at[0], x_recv.at[g]).wait_recv()

    def bulk_sent():
        @pl.when(c == 0)
        def _():
            bulk(xs, x_send.at[0], x_recv.at[0]).wait_send()

        @pl.when(c == 1)
        def _():
            bulk(ys.at[pl.ds(0, 3 * size // 2)], x_send.at[0], x_recv.at[0]).wait_send()

    @pl.when(c == 0)
    def _():
        for q in range(5):
            x_copy(q).start()

    @pl.when(c == 1)
    def _():
        for q in range(3):
            y_copy(q).start()

    up_next = has_below & has_above
    up_waits = place > 1
    down_next = has_above & has_below
    down_waits = place < line - 2

    @pl.when(up_next & jnp.logical_not(up_waits))
    def _():
        signal(relay.at[0], above)

    @pl.when(down_next & jnp.logical_not(down_waits))
    def _():
        signal(relay.at[1], below)

    def everyone():
        @pl.when(up_waits)
        def _():
            pl.semaphore_wait(relay.at[0], 1)

        @pl.when(up_waits & up_next)
        def _():
            signal(relay.at[0], above)

        @pl.when(down_waits)
        def _():
            pl.semaphore_wait(relay.at[1], 1)

        @pl.when(down_waits & down_next)
        def _():
            signal(relay.at[1], below)

        signal(relay.at[3], side)
        pl.semaphore_wait(relay.at[3], 1)
        signal(relay.at[2], across)

    half = part.shape[0] // 2
    chunk = half // mates
    mine = pl.ds(parity * half, half)
    his = pl.ds((1 - parity) * half, half)

    def piece(idx):
        return pl.ds(pl.multiple_of(parity * half + idx * chunk, 8), chunk)

    own = piece(h)

    def g_pair():
        return push(part.at[his], pair_in, g_send.at[0], g_recv.at[0], partner)

    def g_ring(k):
        return push(part.at[piece(mate(k))], ring_in.at[k], g_send.at[0],
                    g_recv.at[1], at(mate(k), c))

    def g_cross():
        return push(gram.at[own], gram.at[own], g_send.at[0], g_recv.at[2], (side[0], other))

    held = piece(h + c * (1 - 2 * lax.rem(h, 2)))

    def g_gather(k):
        return push(gram.at[held], gram.at[held], g_send.at[1], g_recv.at[3], at(mate(k), c))

    def g_half(rows):
        return push(gram.at[rows], gram.at[rows], g_send.at[1], g_recv.at[4], partner)

    def amount(ref, send_sem, recv_sem):
        return push(ref, ref, send_sem, recv_sem, partner)

    owners = range(mates)
    split = mates // 2
    rows_chunk = size // mates

    def rows_at(offset, count):
        return pl.ds(pl.multiple_of(offset, 8), count)

    y_mine = rows_at(parity * size, size)
    y_his = rows_at((1 - parity) * size, size)

    def y_piece(idx):
        return rows_at(parity * size + idx * rows_chunk, rows_chunk)

    def y_pair(q):
        if q < 2:
            src, dst = xy.at[q, y_his], xy_pair.at[q]
        else:
            rows = rows_at((1 - parity) * size + (q - 2) * part_rows, part_rows)
            src, dst = xy.at[:, rows], xy_pair.at[:, pl.ds((q - 2) * part_rows, part_rows)]
        return push(src, dst, y_send.at[0], y_recv.at[q % 2], partner)

    def y_merge(q):
        if q < 2:
            xy[q, y_mine] = xy[q, y_mine] + xy_pair[q]
        else:
            rows = rows_at(parity * size + (q - 2) * part_rows, part_rows)
            span = pl.ds((q - 2) * part_rows, part_rows)
            xy[:, rows] = xy[:, rows] + xy_pair[:, span]

    near, far, share, lend, final = range(2, 7)

    def y_near(j):
        return push(xy.at[c, y_piece(j)], xy_ring.at[0, h], y_send.at[1],
                    y_recv.at[near], at(j, c))

    def y_far(j):
        return push(xy.at[other, y_piece(j)], xy_ring.at[1, h], y_send.at[0],
                    y_recv.at[far], at(j, other))

    def y_share(j):
        view = xy_all.at[c, y_piece(h)]
        return push(view, view, y_send.at[1], y_recv.at[share], at(j, c))

    def y_lend(j, side_core=0):
        view = xy_all.at[c, y_piece(h)]
        row = j * 2 + (1 - parity if side_core else parity)
        return push(view, view, y_send.at[1], y_recv.at[lend], (row, other))

    def y_half(which, plane, rows):
        view = xy_all.at[plane, rows]
        return push(view, view, y_send.at[2], y_recv.at[final + which], partner)

    def unless_self(j, step):
        @pl.when(h != j)
        def _():
            step()

    def scatter(q):
        y_pair(q).wait_recv()
        y_merge(q)
        if q in (1, 3):
            for j in owners:
                y_far(j).start()
        if q != 1:
            for j in owners:
                if q == 0 or (j >= split) == (q == 3):
                    unless_self(j, y_near(j).start)

    def meet(q):
        if q < 2:
            xy[q] = across_rows(xs[:, early], ys[q * size:(q + 1) * size, early])
        else:
            groups = (top, bottom)[q - 2]
            value = across_rows(
                jnp.concatenate([xs[rows, late] for rows in groups], axis=0), ys[:, late])
            for g, rows in enumerate(groups):
                block = value[g * part_rows:(g + 1) * part_rows]
                xy[0, rows] = block[:, :size]
                xy[1, rows] = block[:, size:]
        y_pair(q).start()

    @pl.when(c == 0)
    def _():
        for q in range(2):
            load_copy(q, xs).wait()
            span = early if q == 0 else late
            strip = across_rows(xs[:size, span], xs[:, span])
            rest = across_rows(xs[size:, span], xs[size:, span])
            if q == 0:
                part[:size] = strip[:, :size]
                part[size:2 * size] = strip[:, size:]
                part[2 * size:] = rest
            else:
                part[:size] = part[:size] + strip[:, :size]
                part[size:2 * size] = part[size:2 * size] + strip[:, size:]
                part[2 * size:] = part[2 * size:] + rest
        g_pair().start()

    everyone()

    @pl.when(c == 0)
    def _():
        g_pair().wait_recv()
        part[mine] = part[mine] + pair_in[...]
        for k in range(1, mates):
            g_ring(k).start()
        amount(ring_in.at[pl.ds(1, mates - 1)], g_send.at[0], g_recv.at[1]).wait_recv()
        total = part[own]
        for k in range(1, mates):
            total = total + ring_in[k]
        gram[own] = total
        g_cross().start()

    @pl.when(c == 1)
    def _():
        for q in range(2):
            load_copy(q, ys).wait()
        x_group_wait(0)
        meet(2)
        pl.semaphore_wait(relay.at[2], 1)
        scatter(2)
        amount(gram.at[held], g_send.at[0], g_recv.at[2]).wait_recv()

    for k in range(1, mates):
        g_gather(k).start()

    @pl.when(c == 0)
    def _():
        y_copy(0).wait_recv()
        meet(0)

    @pl.when(c == 1)
    def _():
        x_group_wait(1)
        meet(3)
        scatter(3)

    amount(gram.at[pl.ds(0, (mates - 1) * chunk)], g_send.at[1], g_recv.at[3]).wait_recv()
    g_half(mine).start()

    @pl.when(c == 0)
    def _():
        scatter(0)

    g_half(his).wait_recv()

    eye = (lax.broadcasted_iota(jnp.int32, (size, size), 0)
           == lax.broadcasted_iota(jnp.int32, (size, size), 1)).astype(jnp.float32)
    first[:, :size] = gram[:size]
    first[:, size:2 * size] = gram[size:2 * size]
    first[:, 2 * size:] = eye

    def on_plane(plane, step):
        @pl.when(c == plane)
        def _():
            step()

    def meet_last():
        x_copy(5).start()
        y_copy(1).wait_recv()
        meet(1)

    def scatter_last():
        pl.semaphore_wait(relay.at[2], 1)
        scatter(1)
        for q in range(6, 9):
            x_copy(q).start()

    def gather():
        amount(xy_ring.at[0, pl.ds(0, mates - 1)], y_send.at[1], y_recv.at[near]).wait_recv()
        amount(xy_ring.at[1], y_send.at[0], y_recv.at[far]).wait_recv()
        total = xy[c, y_piece(h)]
        for k in range(1, mates):
            total = total + xy_ring[0, mate(k)]
        for j in range(mates):
            total = total + xy_ring[1, j]
        xy_all[c, y_piece(h)] = total
        for j in range(mates):
            unless_self(j, y_share(j).start)

        @pl.when(c == 0)
        def _():
            for j in range(mates):
                y_lend(j).start()

        @pl.when((c == 1) & (parity == 0))
        def _():
            for j in range(mates):
                for core in range(2):
                    y_lend(j, core).start()

    eliminate(first, {
        0: lambda: on_plane(0, meet_last),
        2: lambda: on_plane(0, scatter_last),
        7: lambda: on_plane(1, gather),
    })

    upper = first[:, size:2 * size]
    cross = contract(upper, first[:, size:], ((0,), (0,)))
    second[:, :size] = gram[2 * size:] - cross[:, :size]
    second[:, size:2 * size] = -cross[:, size:]
    second[:, 2 * size:] = eye
    eliminate(second, {
        3: lambda: on_plane(0, gather),
    })

    inverse[:size, :size] = first[:, 2 * size:]
    inverse[:size, size:] = jnp.zeros((size, size), jnp.float32)
    inverse[size:] = second[:, size:]
    own_rows = pl.ds(pl.multiple_of(c * size, size), size)
    factors[:size] = inverse[own_rows]
    factors[size:] = contract(inverse[...], inverse[...], ((0,), (0,)))

    def products(lo, count):
        span = pl.ds(lo * eighth, count * eighth)
        q_ref[:, span] = product(factors[:size], xs[:, span]) * scaling
        z_ref[:, span] = product(factors[size:], xs[:, span])

    keep = (lax.broadcasted_iota(jnp.int32, (size, size), 0)
            <= lax.broadcasted_iota(jnp.int32, (size, size), 1))

    def trail(lo, count):
        span = cols(lo, count)
        tail_ref[:, span] = ys[own_rows, span] - contract(
            xy_all[c], z_ref[:, span], ((0,), (0,)))

    @pl.when(c == 0)
    def _():
        tri_ref[:, :size] = jnp.where(keep, first[:, :size], 0.0) / scaling
        tri_ref[:, size:2 * size] = first[:, size:2 * size] / scaling
        y_copy(2).wait_recv()

    @pl.when(c == 1)
    def _():
        tri_ref[:, :size] = jnp.zeros((size, size), jnp.float32)
        tri_ref[:, size:2 * size] = jnp.where(keep, second[:, :size], 0.0) / scaling

    inv_ref[...] = factors[:size]
    def rows_of(count):
        return xy_all.at[0, pl.ds(0, count * rows_chunk)]

    def take_own():
        amount(rows_of(mates - 1), y_send.at[1], y_recv.at[share]).wait_recv()
        y_half(0, c, y_mine).start()

    def take_other():
        amount(rows_of(mates), y_send.at[1], y_recv.at[lend]).wait_recv()

    def sent(pieces_sent):
        rows = pieces_sent * rows_chunk // 2
        amount(xy.at[:, pl.ds(0, rows)], y_send.at[1], y_recv.at[0]).wait_send()

    def all_sent():
        amount(gram.at[pl.ds(0, (mates - 1) * chunk + half)], g_send.at[1],
               g_recv.at[0]).wait_send()
        amount(part, y_send.at[0], y_recv.at[0]).wait_send()
        bulk_sent()
        sum_ref[c] = xy_all[c]

    products(4, 4)

    @pl.when(c == 0)
    def _():
        products(0, 4)
        amount(part, g_send.at[0], g_recv.at[0]).wait_send()
        take_own()
        y_half(0, c, y_his).wait_recv()
        sum_ref[1, size:] = jnp.zeros((size, size), jnp.float32)
        trail(0, 8)
        all_sent()
        amount(xy_pair.at[0], y_send.at[2], y_recv.at[0]).wait_send()
        sent(3 * mates - 2)
        take_other()
        sum_ref[1, :size] = xy_all[1, :size]

    @pl.when(c == 1)
    def _():
        take_own()
        for g in range(2, 4):
            x_group_wait(g)
        products(0, 4)
        take_other()
        y_half(1, other, y_mine).start()
        y_half(0, c, y_his).wait_recv()
        trail(0, 8)
        all_sent()

        @pl.when(parity == 0)
        def _():
            sent(4 * mates - 2)

        @pl.when(parity == 1)
        def _():
            sent(2 * mates - 2)

        y_half(1, other, y_his).wait_recv()
        sum_ref[0] = xy_all[0]
        amount(xy_pair, y_send.at[2], y_recv.at[0]).wait_send()


def finish_kernel(scaling, q_in, tail_in, tri_in, inv_ref, sum_ref,
                  ortho_ref, tri_ref, trail_ref, right, sems):
    size = tri_in.shape[0]

    def out(k, src, dst):
        return pltpu.make_async_copy(src, dst, sems.at[k])

    copies = [
        out(0, q_in, ortho_ref),
        out(1, tail_in, trail_ref),
        out(2, tri_in, tri_ref.at[:, :2 * size]),
        out(3, right, tri_ref.at[:, 2 * size:]),
    ]
    for copy in copies[:3]:
        copy.start()
    right[:, :size] = product(inv_ref[...], sum_ref[0]) / scaling
    right[:, size:] = product(inv_ref[...], sum_ref[1]) / scaling
    copies[3].start()
    for copy in copies:
        copy.wait()


def fused(columns):
    row_count = lax.axis_size("rows")
    width = columns.shape[1]
    scaling = math.sqrt(width * row_count)
    size = PANEL
    mates = row_count // 2
    f32 = jnp.float32
    vmem = pl.BlockSpec(memory_space=pltpu.VMEM)
    ortho = jax.ShapeDtypeStruct((size, width), f32)
    triangle = jax.ShapeDtypeStruct((size, 4 * size), f32)
    trailing = ortho
    middle = pl.pallas_call(
        functools.partial(kernel, row_count, scaling),
        out_shape=(
            ortho,
            trailing,
            jax.ShapeDtypeStruct((size, 2 * size), f32),
            jax.ShapeDtypeStruct((size, 2 * size), f32),
            jax.ShapeDtypeStruct((2, 2 * size, size), f32),
        ),
        in_specs=[pl.BlockSpec(memory_space=pltpu.HBM)],
        out_specs=(vmem,) * 5,
        scratch_shapes=[
            pltpu.VMEM((2 * size, width), f32),
            pltpu.VMEM((2 * size, width), f32),
            pltpu.VMEM((3 * size, size), f32),
            pltpu.VMEM((3 * size, size), f32),
            pltpu.VMEM((3 * size // 2, size), f32),
            pltpu.VMEM((mates, 3 * size // row_count, size), f32),
            pltpu.VMEM((size, 3 * size), f32),
            pltpu.VMEM((size, 3 * size), f32),
            pltpu.VMEM((2 * size, 2 * size), f32),
            pltpu.VMEM((3 * size, 2 * size), f32),
            pltpu.VMEM((2 * size, width), f32),
            pltpu.VMEM((2, 2 * size, size), f32),
            pltpu.VMEM((2, size, size), f32),
            pltpu.VMEM((2, mates, size // mates, size), f32),
            pltpu.VMEM((2, 2 * size, size), f32),
            pltpu.SemaphoreType.DMA((2,)),
            pltpu.SemaphoreType.DMA((1,)),
            pltpu.SemaphoreType.DMA((4,)),
            pltpu.SemaphoreType.DMA((2,)),
            pltpu.SemaphoreType.DMA((5,)),
            pltpu.SemaphoreType.DMA((3,)),
            pltpu.SemaphoreType.DMA((8,)),
            pltpu.SemaphoreType.REGULAR((4,)),
        ],
        compiler_params=pltpu.CompilerParams(
            collective_id=0, has_side_effects=True, vmem_limit_bytes=VMEM_BYTES),
    )(pltpu.with_memory_space_constraint(columns, pltpu.HBM))
    return pl.pallas_call(
        functools.partial(finish_kernel, scaling),
        out_shape=(ortho, triangle, trailing),
        in_specs=[vmem] * 5,
        out_specs=(pl.BlockSpec(memory_space=pltpu.HBM),) * 3,
        scratch_shapes=[
            pltpu.VMEM((size, 2 * size), f32),
            pltpu.SemaphoreType.DMA((4,)),
        ],
        compiler_params=pltpu.CompilerParams(vmem_limit_bytes=VMEM_BYTES),
    )(*middle)


def inverse_lower(lower):
    identity = jnp.eye(lower.shape[0], dtype=lower.dtype)
    return lax.linalg.triangular_solve(lower, identity, left_side=True, lower=True)


def summed(partial_term):
    return lax.psum(partial_term, "rows")


def general(columns):
    col_count = lax.axis_size("cols")
    col_index = lax.axis_index("cols")
    scaling = math.sqrt(columns.shape[1] * lax.axis_size("rows"))
    local_rows = lax.all_gather(columns, "cols", axis=0, tiled=True)
    panel_count = 2 * PANEL
    leading = local_rows[:panel_count]
    gram_strip = summed(product(leading, local_rows.T))
    lower_both = jnp.linalg.cholesky(gram_strip[:, :panel_count])
    inverse_both = inverse_lower(lower_both)
    orthonormal = product(inverse_both, leading)
    coupling = product(inverse_both, gram_strip[:, panel_count:])
    trailing = local_rows[panel_count:] - product(coupling.T, orthonormal)
    triangle = jnp.concatenate([lower_both.T, coupling], axis=1)
    orthonormal = orthonormal * scaling
    triangle = triangle / scaling

    def own(array):
        count = array.shape[0] // col_count
        return lax.dynamic_slice_in_dim(array, col_index * count, count, 0)

    return (own(orthonormal), own(triangle), own(trailing))


def shards(columns):
    rows = lax.axis_size("rows")
    paired = lax.axis_size("cols") == 2 and columns.shape[0] == 2 * PANEL and columns.shape[1] % (8 * PANEL) == 0
    if paired and rows % 8 == 0 and (2 * PANEL) % (8 * rows) == 0 and (3 * PANEL) % (8 * rows) == 0:
        return fused(columns)
    return general(columns)


def solution(mesh):
    placed = (P("cols", "rows"),)
    return jax.shard_map(
        shards,
        mesh=mesh,
        in_specs=placed,
        out_specs=(P("cols", "rows"), P("cols", None), P("cols", "rows")),
        check_vma=False,
    )
```

```python
import functools
import math

import jax
import jax.numpy as jnp
from jax import lax
from jax.experimental import pallas as pl
from jax.experimental.pallas import tpu as pltpu
from jax.sharding import PartitionSpec as P

PANEL = 128
STRIP = 16
VMEM_BYTES = 20 * 2**20
MESH = pl.DeviceIdType.MESH

precise = lax.Precision.HIGHEST


def product(left, right):
    return jnp.dot(left, right, precision=precise, preferred_element_type=jnp.float32)


def contract(left, right, dims):
    return lax.dot_general(
        left, right, (dims, ((), ())), precision=precise, preferred_element_type=jnp.float32
    )


def across_rows(left, right):
    return contract(left, right, ((1,), (1,)))


def pieces(value):
    first = value.astype(jnp.bfloat16)
    rest = value - first.astype(jnp.float32)
    second = rest.astype(jnp.bfloat16)
    third = (rest - second.astype(jnp.float32)).astype(jnp.bfloat16)
    return first, second, third


def strip_update(left, right, after):
    a, b, c = pieces(left)
    d, e, f = pieces(right)
    lhs = jnp.concatenate([a, a, b, a, c, b], axis=0)
    rhs = jnp.concatenate([d, e, d, f, d, e], axis=0)
    return jnp.dot(lhs.T[after:], rhs, preferred_element_type=jnp.float32)


def spread(value, i):
    return jnp.broadcast_to(value[i:i + 1], value.shape)


def eliminate(ref, hooks):
    size = ref.shape[0]
    lanes = size
    parts = ref.shape[1] // lanes
    tall = STRIP // 2
    below = lax.broadcasted_iota(jnp.int32, (tall, lanes), 0)

    def column(value, j):
        return jnp.broadcast_to(value[:, j:j + 1], (tall, lanes))

    def diagonal(cols):
        value = cols[0]
        for j in range(1, tall):
            value = jnp.where(below == j, cols[j], value)
        return value

    for s in range(size // STRIP):
        at = s * STRIP
        spans = [slice(q * lanes, (q + 1) * lanes) for q in range(parts)]
        upper = [ref[at:at + tall, span] for span in spans]
        lower = [ref[at + tall:at + STRIP, span] for span in spans]
        tops = [column(upper[0], at + j) for j in range(tall)]
        lows = [column(lower[0], at + j) for j in range(STRIP)]
        scale_top = lax.rsqrt(diagonal(tops))
        scale_low = lax.rsqrt(diagonal(lows[tall:]))
        upper = [value * scale_top for value in upper]
        lower = [value * scale_low for value in lower]
        for j in range(STRIP):
            own_scale = spread(scale_top if j < tall else scale_low, j % tall)
            lows[j] = lows[j] * scale_low * own_scale
            if j < tall:
                tops[j] = tops[j] * scale_top * own_scale
        for i in range(0, STRIP, 2):
            high = i < tall
            r = i % tall
            cur = tops if high else lows
            rows = upper if high else lower
            corner = spread(cur[i], r)
            edge = spread(cur[i], r + 1)
            minor = corner * spread(cur[i + 1], r + 1) - edge * edge
            inv = lax.rsqrt(corner)
            inv_next = lax.rsqrt(minor) * (corner * inv)
            slope = edge * inv
            col = cur[i] * inv
            col_next = (cur[i + 1] - col * slope) * inv_next
            coef = jnp.where(below > r, col, 0.0)
            coef_next = jnp.where(below > r + 1, col_next, 0.0)
            if high:
                tail = lows[i] * inv
                tail_next = (lows[i + 1] - tail * slope) * inv_next
            for j in range(i + 2, STRIP):
                same = high == (j < tall)
                one = spread(col if same else tail, j % tall)
                two = spread(col_next if same else tail_next, j % tall)
                if same:
                    cur[j] = (cur[j] - coef * one) - coef_next * two
                if high:
                    lows[j] = (lows[j] - tail * one) - tail_next * two
            for q in range(parts):
                row = spread(rows[q], r) * inv
                rest = rows[q] - coef * row
                row_next = spread(rest, r + 1) * inv_next
                rest = jnp.where(below == r + 1, row_next, rest - coef_next * row_next)
                rows[q] = jnp.where(below == r, row, rest)
                if high:
                    lower[q] = (lower[q] - tail * row) - tail_next * row_next
        rows = [jnp.concatenate([upper[q], lower[q]], axis=0) for q in range(parts)]
        for q in range(parts):
            ref[at:at + STRIP, spans[q]] = rows[q]
        after = at + STRIP
        if after < size:
            update = strip_update(rows[0], jnp.concatenate(rows, axis=1), after)
            ref[after:, :] = ref[after:, :] - update
        if s in hooks:
            hooks[s]()


def kernel(row_count, scaling, x_ref, q_ref, tail_ref, tri_ref, inv_ref, sum_ref,
           xs, ys, part, gram, pair_in, ring_in, first, second, inverse, factors, z_ref,
           xy, xy_pair, xy_ring, xy_all, load, x_send, x_recv, g_send, g_recv,
           y_send, y_recv, relay):
    r = lax.axis_index("rows")
    c = lax.axis_index("cols")
    other = 1 - c
    parity = lax.rem(r, 2)
    h = r // 2
    mates = row_count // 2
    line = mates // 2
    place = h // 2
    partner = (r + 1 - 2 * parity, c)
    across = (r, other)
    side = ((h + 1 - 2 * lax.rem(h, 2)) * 2 + parity, c)
    above = (r + 4, c)
    below = (r - 4, c)
    has_above = place < line - 1
    has_below = place > 0
    size = PANEL
    width = xs.shape[1]
    half_width = width // 2
    eighth = width // 8

    def mate(k):
        return lax.rem(h + k, mates)

    def at(idx, plane):
        return (idx * 2 + parity, plane)

    def push(src, dst, send_sem, recv_sem, target):
        return pltpu.make_async_remote_copy(
            src_ref=src, dst_ref=dst, send_sem=send_sem, recv_sem=recv_sem,
            device_id=target, device_id_type=MESH)

    def signal(sem, target):
        pl.semaphore_signal(sem, inc=1, device_id=target, device_id_type=MESH)

    barrier = pltpu.get_barrier_semaphore()
    for target in (across, partner, side):
        signal(barrier, target)

    @pl.when(has_above)
    def _():
        signal(barrier, above)

    @pl.when(has_below)
    def _():
        signal(barrier, below)

    early = pl.ds(0, half_width)
    late = pl.ds(half_width, half_width)

    def load_copy(q, dst):
        span = early if q == 0 else late
        return pltpu.make_async_copy(x_ref.at[:, span], dst.at[:, span], load.at[q])

    @pl.when(c == 0)
    def _():
        for q in range(2):
            load_copy(q, xs).start()

    @pl.when(c == 1)
    def _():
        for q in range(2):
            load_copy(q, ys).start()

    pl.semaphore_wait(barrier, 3 + has_above.astype(jnp.int32) + has_below.astype(jnp.int32))

    part_rows = size // 2
    top = [pl.ds(q * size, part_rows) for q in range(2)]
    bottom = [pl.ds(q * size + part_rows, part_rows) for q in range(2)]
    every = pl.ds(0, 2 * size)

    def cols(lo, count):
        return pl.ds(lo * eighth, count * eighth)

    x_views = (
        [(rows, late) for rows in top]
        + [(rows, late) for rows in bottom]
        + [(every, cols(0, 1)), (pl.ds(0, size), cols(1, 1)), (pl.ds(size, size), cols(1, 1)),
           (every, cols(2, 1)), (every, cols(3, 1))]
    )
    y_views = [(pl.ds(0, size), early), (pl.ds(size, size), early), (pl.ds(0, size), late)]

    x_group = (0, 0, 1, 1, 2, 2, 2, 3, 3)

    def x_copy(q):
        return push(x_ref.at[x_views[q]], xs.at[x_views[q]], x_send.at[0],
                    x_recv.at[x_group[q]], across)

    def y_copy(q):
        return push(x_ref.at[y_views[q]], ys.at[y_views[q]], x_send.at[0], x_recv.at[q], across)

    def bulk(ref, send_sem, recv_sem):
        return push(ref, ref, send_sem, recv_sem, across)

    x_sizes = ((size, late), (size, late), (2 * size, cols(0, 2)),
               (2 * size, cols(2, 2)))

    def x_group_wait(g):
        rows, span = x_sizes[g]
        bulk(xs.at[pl.ds(0, rows), span], x_send.at[0], x_recv.at[g]).wait_recv()

    def bulk_sent():
        @pl.when(c == 0)
        def _():
            bulk(xs, x_send.at[0], x_recv.at[0]).wait_send()

        @pl.when(c == 1)
        def _():
            bulk(ys.at[pl.ds(0, 3 * size // 2)], x_send.at[0], x_recv.at[0]).wait_send()

    @pl.when(c == 0)
    def _():
        for q in range(5):
            x_copy(q).start()

    @pl.when(c == 1)
    def _():
        for q in range(3):
            y_copy(q).start()

    up_next = has_below & has_above
    up_waits = place > 1
    down_next = has_above & has_below
    down_waits = place < line - 2

    @pl.when(up_next & jnp.logical_not(up_waits))
    def _():
        signal(relay.at[0], above)

    @pl.when(down_next & jnp.logical_not(down_waits))
    def _():
        signal(relay.at[1], below)

    def everyone():
        @pl.when(up_waits)
        def _():
            pl.semaphore_wait(relay.at[0], 1)

        @pl.when(up_waits & up_next)
        def _():
            signal(relay.at[0], above)

        @pl.when(down_waits)
        def _():
            pl.semaphore_wait(relay.at[1], 1)

        @pl.when(down_waits & down_next)
        def _():
            signal(relay.at[1], below)

        signal(relay.at[3], side)
        pl.semaphore_wait(relay.at[3], 1)
        signal(relay.at[2], across)

    half = part.shape[0] // 2
    chunk = half // mates
    mine = pl.ds(parity * half, half)
    his = pl.ds((1 - parity) * half, half)

    def piece(idx):
        return pl.ds(pl.multiple_of(parity * half + idx * chunk, 8), chunk)

    own = piece(h)

    def g_pair():
        return push(part.at[his], pair_in, g_send.at[0], g_recv.at[0], partner)

    def g_ring(k):
        return push(part.at[piece(mate(k))], ring_in.at[k], g_send.at[0],
                    g_recv.at[1], at(mate(k), c))

    def g_cross():
        return push(gram.at[own], gram.at[own], g_send.at[0], g_recv.at[2], (side[0], other))

    held = piece(h + c * (1 - 2 * lax.rem(h, 2)))

    def g_gather(k):
        return push(gram.at[held], gram.at[held], g_send.at[1], g_recv.at[3], at(mate(k), c))

    def g_half(rows):
        return push(gram.at[rows], gram.at[rows], g_send.at[1], g_recv.at[4], partner)

    def amount(ref, send_sem, recv_sem):
        return push(ref, ref, send_sem, recv_sem, partner)

    owners = range(mates)
    split = mates // 2
    rows_chunk = size // mates

    def rows_at(offset, count):
        return pl.ds(pl.multiple_of(offset, 8), count)

    y_mine = rows_at(parity * size, size)
    y_his = rows_at((1 - parity) * size, size)

    def y_piece(idx):
        return rows_at(parity * size + idx * rows_chunk, rows_chunk)

    def y_pair(q):
        if q < 2:
            src, dst = xy.at[q, y_his], xy_pair.at[q]
        else:
            rows = rows_at((1 - parity) * size + (q - 2) * part_rows, part_rows)
            src, dst = xy.at[:, rows], xy_pair.at[:, pl.ds((q - 2) * part_rows, part_rows)]
        return push(src, dst, y_send.at[0], y_recv.at[q % 2], partner)

    def y_merge(q):
        if q < 2:
            xy[q, y_mine] = xy[q, y_mine] + xy_pair[q]
        else:
            rows = rows_at(parity * size + (q - 2) * part_rows, part_rows)
            span = pl.ds((q - 2) * part_rows, part_rows)
            xy[:, rows] = xy[:, rows] + xy_pair[:, span]

    near, far, share, lend, final = range(2, 7)

    def y_near(j):
        return push(xy.at[c, y_piece(j)], xy_ring.at[0, h], y_send.at[1],
                    y_recv.at[near], at(j, c))

    def y_far(j):
        return push(xy.at[other, y_piece(j)], xy_ring.at[1, h], y_send.at[0],
                    y_recv.at[far], at(j, other))

    def y_share(j):
        view = xy_all.at[c, y_piece(h)]
        return push(view, view, y_send.at[1], y_recv.at[share], at(j, c))

    def y_lend(j, side_core=0):
        view = xy_all.at[c, y_piece(h)]
        row = j * 2 + (1 - parity if side_core else parity)
        return push(view, view, y_send.at[1], y_recv.at[lend], (row, other))

    def y_half(which, plane, rows):
        view = xy_all.at[plane, rows]
        return push(view, view, y_send.at[2], y_recv.at[final + which], partner)

    def unless_self(j, step):
        @pl.when(h != j)
        def _():
            step()

    def scatter(q):
        y_pair(q).wait_recv()
        y_merge(q)
        if q in (1, 3):
            for j in owners:
                y_far(j).start()
        if q != 1:
            for j in owners:
                if q == 0 or (j >= split) == (q == 3):
                    unless_self(j, y_near(j).start)

    def meet(q):
        if q < 2:
            xy[q] = across_rows(xs[:, early], ys[q * size:(q + 1) * size, early])
        else:
            groups = (top, bottom)[q - 2]
            value = across_rows(
                jnp.concatenate([xs[rows, late] for rows in groups], axis=0), ys[:, late])
            for g, rows in enumerate(groups):
                block = value[g * part_rows:(g + 1) * part_rows]
                xy[0, rows] = block[:, :size]
                xy[1, rows] = block[:, size:]
        y_pair(q).start()

    @pl.when(c == 0)
    def _():
        for q in range(2):
            load_copy(q, xs).wait()
            span = early if q == 0 else late
            strip = across_rows(xs[:size, span], xs[:, span])
            rest = across_rows(xs[size:, span], xs[size:, span])
            if q == 0:
                part[:size] = strip[:, :size]
                part[size:2 * size] = strip[:, size:]
                part[2 * size:] = rest
            else:
                part[:size] = part[:size] + strip[:, :size]
                part[size:2 * size] = part[size:2 * size] + strip[:, size:]
                part[2 * size:] = part[2 * size:] + rest
        g_pair().start()

    everyone()

    @pl.when(c == 0)
    def _():
        g_pair().wait_recv()
        part[mine] = part[mine] + pair_in[...]
        for k in range(1, mates):
            g_ring(k).start()
        amount(ring_in.at[pl.ds(1, mates - 1)], g_send.at[0], g_recv.at[1]).wait_recv()
        total = part[own]
        for k in range(1, mates):
            total = total + ring_in[k]
        gram[own] = total
        g_cross().start()

    @pl.when(c == 1)
    def _():
        for q in range(2):
            load_copy(q, ys).wait()
        x_group_wait(0)
        meet(2)
        pl.semaphore_wait(relay.at[2], 1)
        scatter(2)
        amount(gram.at[held], g_send.at[0], g_recv.at[2]).wait_recv()

    for k in range(1, mates):
        g_gather(k).start()

    @pl.when(c == 0)
    def _():
        y_copy(0).wait_recv()
        meet(0)

    @pl.when(c == 1)
    def _():
        x_group_wait(1)
        meet(3)
        scatter(3)

    amount(gram.at[pl.ds(0, (mates - 1) * chunk)], g_send.at[1], g_recv.at[3]).wait_recv()
    g_half(mine).start()

    @pl.when(c == 0)
    def _():
        scatter(0)

    g_half(his).wait_recv()

    eye = (lax.broadcasted_iota(jnp.int32, (size, size), 0)
           == lax.broadcasted_iota(jnp.int32, (size, size), 1)).astype(jnp.float32)
    first[:, :size] = gram[:size]
    first[:, size:2 * size] = gram[size:2 * size]
    first[:, 2 * size:] = eye

    def on_plane(plane, step):
        @pl.when(c == plane)
        def _():
            step()

    def meet_last():
        for q in range(5, 7):
            x_copy(q).start()
        y_copy(1).wait_recv()
        meet(1)

    def scatter_last():
        pl.semaphore_wait(relay.at[2], 1)
        scatter(1)
        for q in range(7, 9):
            x_copy(q).start()

    def gather():
        amount(xy_ring.at[0, pl.ds(0, mates - 1)], y_send.at[1], y_recv.at[near]).wait_recv()
        amount(xy_ring.at[1], y_send.at[0], y_recv.at[far]).wait_recv()
        total = xy[c, y_piece(h)]
        for k in range(1, mates):
            total = total + xy_ring[0, mate(k)]
        for j in range(mates):
            total = total + xy_ring[1, j]
        xy_all[c, y_piece(h)] = total
        for j in range(mates):
            unless_self(j, y_share(j).start)

        @pl.when(c == 0)
        def _():
            for j in range(mates):
                y_lend(j).start()

        @pl.when((c == 1) & (parity == 0))
        def _():
            for j in range(mates):
                for core in range(2):
                    y_lend(j, core).start()

    eliminate(first, {
        0: lambda: on_plane(0, meet_last),
        2: lambda: on_plane(0, scatter_last),
        7: lambda: on_plane(1, gather),
    })

    upper = first[:, size:2 * size]
    cross = contract(upper, first[:, size:], ((0,), (0,)))
    second[:, :size] = gram[2 * size:] - cross[:, :size]
    second[:, size:2 * size] = -cross[:, size:]
    second[:, 2 * size:] = eye
    eliminate(second, {
        3: lambda: on_plane(0, gather),
    })

    inverse[:size, :size] = first[:, 2 * size:]
    inverse[:size, size:] = jnp.zeros((size, size), jnp.float32)
    inverse[size:] = second[:, size:]
    own_rows = pl.ds(pl.multiple_of(c * size, size), size)
    factors[:size] = inverse[own_rows]
    factors[size:] = contract(inverse[...], inverse[...], ((0,), (0,)))

    def products(lo, count):
        span = pl.ds(lo * eighth, count * eighth)
        q_ref[:, span] = product(factors[:size], xs[:, span]) * scaling
        z_ref[:, span] = product(factors[size:], xs[:, span])

    keep = (lax.broadcasted_iota(jnp.int32, (size, size), 0)
            <= lax.broadcasted_iota(jnp.int32, (size, size), 1))

    def trail(lo, count):
        span = cols(lo, count)
        tail_ref[:, span] = ys[own_rows, span] - contract(
            xy_all[c], z_ref[:, span], ((0,), (0,)))

    @pl.when(c == 0)
    def _():
        tri_ref[:, :size] = jnp.where(keep, first[:, :size], 0.0) / scaling
        tri_ref[:, size:2 * size] = first[:, size:2 * size] / scaling
        y_copy(2).wait_recv()

    @pl.when(c == 1)
    def _():
        tri_ref[:, :size] = jnp.zeros((size, size), jnp.float32)
        tri_ref[:, size:2 * size] = jnp.where(keep, second[:, :size], 0.0) / scaling

    inv_ref[...] = factors[:size]
    def rows_of(count):
        return xy_all.at[0, pl.ds(0, count * rows_chunk)]

    def take_own():
        amount(rows_of(mates - 1), y_send.at[1], y_recv.at[share]).wait_recv()
        y_half(0, c, y_mine).start()

    def take_other():
        amount(rows_of(mates), y_send.at[1], y_recv.at[lend]).wait_recv()

    def sent(pieces_sent):
        rows = pieces_sent * rows_chunk // 2
        amount(xy.at[:, pl.ds(0, rows)], y_send.at[1], y_recv.at[0]).wait_send()

    def early_sent():
        amount(gram.at[pl.ds(0, (mates - 1) * chunk + half)], g_send.at[1],
               g_recv.at[0]).wait_send()
        amount(part, y_send.at[0], y_recv.at[0]).wait_send()

    products(4, 4)

    @pl.when(c == 0)
    def _():
        products(0, 4)
        amount(part, g_send.at[0], g_recv.at[0]).wait_send()
        early_sent()
        sum_ref[1, size:] = jnp.zeros((size, size), jnp.float32)
        take_own()
        y_half(0, c, y_his).wait_recv()
        trail(0, 8)
        bulk_sent()
        sent(3 * mates - 2)
        sum_ref[c] = xy_all[c]
        amount(xy_pair.at[0], y_send.at[2], y_recv.at[0]).wait_send()
        take_other()
        sum_ref[1, :size] = xy_all[1, :size]

    @pl.when(c == 1)
    def _():
        take_own()
        early_sent()
        bulk_sent()

        @pl.when(parity == 0)
        def _():
            sent(4 * mates - 2)

        @pl.when(parity == 1)
        def _():
            sent(2 * mates - 2)

        x_group_wait(2)
        x_group_wait(3)
        products(0, 4)
        take_other()
        y_half(1, other, y_mine).start()
        y_half(0, c, y_his).wait_recv()
        trail(0, 8)
        sum_ref[c] = xy_all[c]
        y_half(1, other, y_his).wait_recv()
        sum_ref[0] = xy_all[0]
        amount(xy_pair, y_send.at[2], y_recv.at[0]).wait_send()


def finish_kernel(scaling, q_in, tail_in, tri_in, inv_ref, sum_ref,
                  ortho_ref, tri_ref, trail_ref, right, sems):
    size = tri_in.shape[0]

    def out(k, src, dst):
        return pltpu.make_async_copy(src, dst, sems.at[k])

    copies = [
        out(0, q_in, ortho_ref),
        out(1, tail_in, trail_ref),
        out(2, tri_in, tri_ref.at[:, :2 * size]),
        out(3, right, tri_ref.at[:, 2 * size:]),
    ]
    for copy in copies[:3]:
        copy.start()
    right[:, :size] = product(inv_ref[...], sum_ref[0]) / scaling
    right[:, size:] = product(inv_ref[...], sum_ref[1]) / scaling
    copies[3].start()
    for copy in copies:
        copy.wait()


def fused(columns):
    row_count = lax.axis_size("rows")
    width = columns.shape[1]
    scaling = math.sqrt(width * row_count)
    size = PANEL
    mates = row_count // 2
    f32 = jnp.float32
    vmem = pl.BlockSpec(memory_space=pltpu.VMEM)
    ortho = jax.ShapeDtypeStruct((size, width), f32)
    triangle = jax.ShapeDtypeStruct((size, 4 * size), f32)
    trailing = ortho
    middle = pl.pallas_call(
        functools.partial(kernel, row_count, scaling),
        out_shape=(
            ortho,
            trailing,
            jax.ShapeDtypeStruct((size, 2 * size), f32),
            jax.ShapeDtypeStruct((size, 2 * size), f32),
            jax.ShapeDtypeStruct((2, 2 * size, size), f32),
        ),
        in_specs=[pl.BlockSpec(memory_space=pltpu.HBM)],
        out_specs=(vmem,) * 5,
        scratch_shapes=[
            pltpu.VMEM((2 * size, width), f32),
            pltpu.VMEM((2 * size, width), f32),
            pltpu.VMEM((3 * size, size), f32),
            pltpu.VMEM((3 * size, size), f32),
            pltpu.VMEM((3 * size // 2, size), f32),
            pltpu.VMEM((mates, 3 * size // row_count, size), f32),
            pltpu.VMEM((size, 3 * size), f32),
            pltpu.VMEM((size, 3 * size), f32),
            pltpu.VMEM((2 * size, 2 * size), f32),
            pltpu.VMEM((3 * size, 2 * size), f32),
            pltpu.VMEM((2 * size, width), f32),
            pltpu.VMEM((2, 2 * size, size), f32),
            pltpu.VMEM((2, size, size), f32),
            pltpu.VMEM((2, mates, size // mates, size), f32),
            pltpu.VMEM((2, 2 * size, size), f32),
            pltpu.SemaphoreType.DMA((2,)),
            pltpu.SemaphoreType.DMA((1,)),
            pltpu.SemaphoreType.DMA((4,)),
            pltpu.SemaphoreType.DMA((2,)),
            pltpu.SemaphoreType.DMA((5,)),
            pltpu.SemaphoreType.DMA((3,)),
            pltpu.SemaphoreType.DMA((8,)),
            pltpu.SemaphoreType.REGULAR((4,)),
        ],
        compiler_params=pltpu.CompilerParams(
            collective_id=0, has_side_effects=True, vmem_limit_bytes=VMEM_BYTES),
    )(pltpu.with_memory_space_constraint(columns, pltpu.HBM))
    return pl.pallas_call(
        functools.partial(finish_kernel, scaling),
        out_shape=(ortho, triangle, trailing),
        in_specs=[vmem] * 5,
        out_specs=(pl.BlockSpec(memory_space=pltpu.HBM),) * 3,
        scratch_shapes=[
            pltpu.VMEM((size, 2 * size), f32),
            pltpu.SemaphoreType.DMA((4,)),
        ],
        compiler_params=pltpu.CompilerParams(vmem_limit_bytes=VMEM_BYTES),
    )(*middle)


def inverse_lower(lower):
    identity = jnp.eye(lower.shape[0], dtype=lower.dtype)
    return lax.linalg.triangular_solve(lower, identity, left_side=True, lower=True)


def summed(partial_term):
    return lax.psum(partial_term, "rows")


def general(columns):
    col_count = lax.axis_size("cols")
    col_index = lax.axis_index("cols")
    scaling = math.sqrt(columns.shape[1] * lax.axis_size("rows"))
    local_rows = lax.all_gather(columns, "cols", axis=0, tiled=True)
    panel_count = 2 * PANEL
    leading = local_rows[:panel_count]
    gram_strip = summed(product(leading, local_rows.T))
    lower_both = jnp.linalg.cholesky(gram_strip[:, :panel_count])
    inverse_both = inverse_lower(lower_both)
    orthonormal = product(inverse_both, leading)
    coupling = product(inverse_both, gram_strip[:, panel_count:])
    trailing = local_rows[panel_count:] - product(coupling.T, orthonormal)
    triangle = jnp.concatenate([lower_both.T, coupling], axis=1)
    orthonormal = orthonormal * scaling
    triangle = triangle / scaling

    def own(array):
        count = array.shape[0] // col_count
        return lax.dynamic_slice_in_dim(array, col_index * count, count, 0)

    return (own(orthonormal), own(triangle), own(trailing))


def shards(columns):
    rows = lax.axis_size("rows")
    paired = lax.axis_size("cols") == 2 and columns.shape[0] == 2 * PANEL and columns.shape[1] % (8 * PANEL) == 0
    if paired and rows % 8 == 0 and (2 * PANEL) % (8 * rows) == 0 and (3 * PANEL) % (8 * rows) == 0:
        return fused(columns)
    return general(columns)


def solution(mesh):
    placed = (P("cols", "rows"),)
    return jax.shard_map(
        shards,
        mesh=mesh,
        in_specs=placed,
        out_specs=(P("cols", "rows"), P("cols", None), P("cols", "rows")),
        check_vma=False,
    )
```
